32 devices in a mesh: occ: 8 (over z, core), aux: 4 (over y, x).
Axes of the slice: x: 2, y: 2, z: 4, core: 2. Of those that a mesh axis runs over, the one named last changes fastest.
Arguments:
- integrals: bfloat16 [2048, 256, 512], P('aux', 'occ'), may hold values from -1.1953125 to 1.1953125
- metric: bfloat16 [2048, 2048], replicated, may hold values from -0.125 to 0.125
- e_occ: float32 [256], replicated, may hold values from -2 to -0.3
- e_vir: float32 [512], replicated, may hold values from 0.2 to 3
- partner: int32 [256, 2], P(('occ', 'aux')), may hold values from 0 to 7
- screen: int32 [256, 2], P(('occ', 'aux')), may hold values from 0 to 1
Outputs:
- gradient: bfloat16 [2048, 256, 512], P(None, ('occ', 'aux'))
- density: float32 [512, 512], P('occ')
The draws below stay inside these ranges and needn't reach their ends.
All inputs are finite; a program needn't handle non-finite values.
Results may differ from the reference program's by a relative error of at most 0.0055.
Values may be sent and summed in bfloat16 or wider, within the bound.
A program may use at most 192 MiB of HBM per device.

```python
import jax
import jax.numpy as jnp
from jax import lax

NOCC = 256
NVIR = 512
NAUX = 2048
ROUNDS = 2
OWN = 8
N_OCC = 8
N_AUX = 4


def draw_screen(key, part):
    first, second = jax.random.split(jax.random.fold_in(key, 17))
    level = jax.random.randint(first, (NOCC // OWN, 1, 1), 1, 5)
    roll = jax.random.randint(second, (NOCC // OWN, OWN, ROUNDS), 0, 4)
    return (roll < level).astype(jnp.int32).reshape(NOCC, ROUNDS)


def touch_ends(entries, rng, low, top_value):
    extent = entries.shape
    place = [jax.random.randint(jax.random.fold_in(rng, axis), (), 0, extent[axis]) for axis in range(len(extent))]
    entries = entries.at[tuple(place)].set(low)
    longest = extent.index(max(extent))
    place[longest] = (place[longest] + 1) % extent[longest]
    return entries.at[tuple(place)].set(top_value)


def level_of(own_key, extent, cuts, smallest, largest):
    def one(dim, parts):
        heights = jax.random.uniform(jax.random.fold_in(jax.random.fold_in(own_key, 6), dim), (parts,), jnp.float32, smallest / len(cuts), largest / len(cuts))
        return jnp.repeat(jnp.exp(heights), extent[dim] // parts).reshape((-1,) + (1,) * (len(extent) - dim - 1))

    gain = one(*cuts[0])
    for cut in cuts[1:]:
        gain = gain * one(*cut)
    return gain


def normal_values(key, extent, spread, most, pieces=(), kind=jnp.bfloat16):
    array = jax.random.normal(key, extent, jnp.float32) * spread
    if len(pieces) > 0:
        array = level_of(key, extent, pieces, -0.22, 0.18) * array
    return jnp.clip(array, min=-most, max=most).astype(kind)


def setup_inputs(seed: int = 0) -> dict:
    keys = jax.random.split(jax.random.key(seed), 7)
    integrals = normal_values(keys[0], (NAUX, NOCC, NVIR), 0.17, 1.1953125, ((0, 4), (1, 8)))
    metric = normal_values(keys[1], (NAUX, NAUX), NAUX ** -0.5, 0.125)
    e_occ = jnp.clip(jax.random.uniform(keys[2], (NOCC,), jnp.float32, -2.0, -0.3), -2.0, -0.3)
    e_vir = jnp.clip(jax.random.uniform(keys[3], (NVIR,), jnp.float32, 0.2, 3.0), 0.2, 3.0)
    partner = touch_ends(jax.random.randint(keys[4], (NOCC, ROUNDS), 0, OWN), jax.random.fold_in(keys[4], 1), 0, OWN - 1).astype(jnp.int32)
    screen = draw_screen(jax.random.fold_in(keys[6], 71), 0)
    return {"integrals": integrals, "metric": metric, "e_occ": e_occ, "e_vir": e_vir, "partner": partner, "screen": screen}


def reference(integrals, metric, e_occ, e_vir, partner, screen):
    groups = N_OCC * N_AUX
    own = NOCC // groups
    flat = integrals.reshape(NAUX, NOCC * NVIR)
    coeff = jnp.dot(metric, flat, preferred_element_type=jnp.float32).astype(jnp.bfloat16).reshape(NAUX, NOCC, NVIR)
    pair_sum = e_vir[:, None] + e_vir[None, :]
    shifts = (1, groups // 2)

    def visit(density, index):
        gamma_row = jnp.zeros((NAUX, NVIR), jnp.float32)
        for rnd in range(ROUNDS):
            source = (index // own - shifts[rnd % 2]) % groups
            other = (source * own + partner[index, rnd]).astype(jnp.int32)
            left = lax.dynamic_index_in_dim(coeff, index, 1, False)
            right = lax.dynamic_index_in_dim(coeff, other, 1, False)
            intersection = lax.dot_general(left, right, (((0,), (0,)), ((), ())), preferred_element_type=jnp.float32)
            gap = pair_sum - e_occ[index] - e_occ[other]
            amp = (screen[index, rnd].astype(jnp.float32) * intersection / gap).astype(jnp.bfloat16)
            gamma_row = gamma_row + lax.dot_general(right, amp, (((1,), (1,)), ((), ())), preferred_element_type=jnp.float32)
            density = density + lax.dot_general(amp, amp, (((1,), (1,)), ((), ())), preferred_element_type=jnp.float32)
        return density, gamma_row.astype(jnp.bfloat16)

    start = jnp.zeros((NVIR, NVIR), jnp.float32)
    density, rows = lax.scan(visit, start, jnp.arange(NOCC, dtype=jnp.int32))
    gradient = jnp.transpose(rows, (1, 0, 2))
    return gradient, density / NOCC
```

```python
import functools

import jax
import jax.numpy as jnp
from jax import lax
from jax.experimental import pallas as pl
from jax.experimental.pallas import tpu as pltpu
from jax.sharding import PartitionSpec as P

NOCC = 256
ROUNDS = 2
BOTH = ("occ", "aux")
NT = (((1,), (1,)), ((), ()))
TN = (((0,), (0,)), ((), ()))

MESH = pl.DeviceIdType.MESH


def amp_kernel(left_at, right_at, kept, e_left, e_right, left, right, col, row, before, amp, density):
    pair = pl.program_id(0)

    @pl.when(pair == 0)
    def _():
        density[...] = before[...]

    @pl.when(kept[pair] != 0)
    def _():
        both = lax.dot_general(left[0], right[0], TN, preferred_element_type=jnp.float32)
        gap = col[...] + row[...] - e_left[pair] - e_right[pair]
        block = (both / gap).astype(jnp.bfloat16)
        amp[0] = block
        density[...] += lax.dot_general(block, block, NT, preferred_element_type=jnp.float32)

    @pl.when(kept[pair] == 0)
    def _():
        amp[0] = jnp.zeros_like(amp[0])


def amplitudes(left, right, left_at, right_at, kept, e_left, e_right, e_vir, before):
    _, naux, nvir = left.shape
    pairs = left_at.shape[0]
    wide = (1, naux, nvir)
    return pl.pallas_call(
        amp_kernel,
        grid_spec=pltpu.PrefetchScalarGridSpec(
            num_scalar_prefetch=5,
            grid=(pairs,),
            in_specs=[
                pl.BlockSpec(wide, lambda m, li, ri, *_: (li[m], 0, 0)),
                pl.BlockSpec(wide, lambda m, li, ri, *_: (ri[m], 0, 0)),
                pl.BlockSpec((nvir, 1), lambda m, *_: (0, 0)),
                pl.BlockSpec((1, nvir), lambda m, *_: (0, 0)),
                pl.BlockSpec((nvir, nvir), lambda m, *_: (0, 0)),
            ],
            out_specs=[
                pl.BlockSpec((1, nvir, nvir), lambda m, *_: (m, 0, 0)),
                pl.BlockSpec((nvir, nvir), lambda m, *_: (0, 0)),
            ],
        ),
        out_shape=[
            jax.ShapeDtypeStruct((pairs, nvir, nvir), jnp.bfloat16),
            jax.ShapeDtypeStruct((nvir, nvir), jnp.float32),
        ],
        cost_estimate=pl.CostEstimate(
            flops=2 * pairs * (naux + nvir) * nvir * nvir,
            bytes_accessed=4 * pairs * naux * nvir,
            transcendentals=0,
        ),
    )(left_at, right_at, kept, e_left, e_right, left, right, e_vir[:, None], e_vir[None, :], before)


def gamma_kernel(own, at0, at1, kept0, kept1, right0, right1, amp0, amp1, out, rows):
    tile = right0.shape[1]
    for i in range(own):
        place = pl.ds(i, tile, stride=own)
        first, second = kept0[i] != 0, kept1[i] != 0

        def term0():
            return lax.dot_general(right0[at0[i]], amp0[i], NT, preferred_element_type=jnp.float32)

        def term1():
            return lax.dot_general(right1[at1[i]], amp1[i], NT, preferred_element_type=jnp.float32)

        def put(value):
            for c in range(rows.shape[0]):
                rows[c, place, :] = value[:, c * 128 : (c + 1) * 128]

        @pl.when(first & second)
        def _():
            put(term0() + term1())

        @pl.when(first & jnp.logical_not(second))
        def _():
            put(term0())

        @pl.when(jnp.logical_not(first) & second)
        def _():
            put(term1())

        @pl.when(jnp.logical_not(first | second))
        def _():
            put(jnp.zeros((tile, out.shape[2]), jnp.float32))

    for c in range(rows.shape[0]):
        block = rows[c].reshape(tile, own, 128)
        out[:, :, c * 128 : (c + 1) * 128] = block.astype(out.dtype)


def gradient(right0, right1, amp0, amp1, at0, at1, kept0, kept1):
    own = amp0.shape[0]
    _, naux, nvir = right0.shape
    tile = min(128, naux)
    full = lambda p, *_: (0, 0, 0)
    return pl.pallas_call(
        functools.partial(gamma_kernel, own),
        grid_spec=pltpu.PrefetchScalarGridSpec(
            num_scalar_prefetch=4,
            grid=(naux // tile,),
            in_specs=[
                pl.BlockSpec((right0.shape[0], tile, nvir), lambda p, *_: (0, p, 0)),
                pl.BlockSpec((right1.shape[0], tile, nvir), lambda p, *_: (0, p, 0)),
                pl.BlockSpec(amp0.shape, full),
                pl.BlockSpec(amp1.shape, full),
            ],
            out_specs=pl.BlockSpec((tile, own, nvir), lambda p, *_: (p, 0, 0)),
            scratch_shapes=[pltpu.VMEM((nvir // 128, tile * own, 128), jnp.float32)],
        ),
        out_shape=jax.ShapeDtypeStruct((naux, own, nvir), jnp.bfloat16),
        cost_estimate=pl.CostEstimate(
            flops=4 * own * naux * nvir * nvir, bytes_accessed=6 * own * naux * nvir, transcendentals=0
        ),
    )(at0, at1, kept0, kept1, right0, right1, amp0, amp1)


def table_kernel(n_occ, n_aux, row, table, send, recv, local):
    groups = n_occ * n_aux
    me = lax.axis_index("occ") * n_aux + lax.axis_index("aux")
    barrier = pltpu.get_barrier_semaphore()

    def place(step):
        other = lax.rem(me + step, groups)
        return (other // n_aux, lax.rem(other, n_aux))

    def greet(step, carry):
        pl.semaphore_signal(barrier, inc=1, device_id=place(step), device_id_type=MESH)
        return carry

    lax.fori_loop(1, groups, greet, 0)
    own = pltpu.make_async_copy(row, table.at[me], local)
    own.start()
    pl.semaphore_wait(barrier, groups - 1)

    def copy(step):
        return pltpu.make_async_remote_copy(
            row, table.at[me], send.at[step], recv.at[step], device_id=place(step), device_id_type=MESH
        )

    def start(step, carry):
        copy(step).start()
        return carry

    def finish(step, carry):
        came = lax.rem(me - step + groups, groups)
        pltpu.make_async_remote_copy(
            row, table.at[came], send.at[step], recv.at[step], device_id=place(step), device_id_type=MESH
        ).wait()
        return carry

    lax.fori_loop(1, groups, start, 0)
    own.wait()
    lax.fori_loop(1, groups, finish, 0)


def everyones(row, n_occ, n_aux):
    groups = n_occ * n_aux
    return pl.pallas_call(
        functools.partial(table_kernel, n_occ, n_aux),
        out_shape=jax.ShapeDtypeStruct((groups,) + row.shape, row.dtype),
        in_specs=[pl.BlockSpec(memory_space=pltpu.VMEM)],
        out_specs=pl.BlockSpec(memory_space=pltpu.VMEM),
        scratch_shapes=[
            pltpu.SemaphoreType.DMA((groups,)),
            pltpu.SemaphoreType.DMA((groups,)),
            pltpu.SemaphoreType.DMA(()),
        ],
        compiler_params=pltpu.CompilerParams(collective_id=0, has_side_effects=True),
    )(row)


def peer_of(i, step, n_aux):
    return i ^ step if n_aux & (n_aux - 1) == 0 else lax.rem(step + n_aux - i, n_aux)


def move_kernel(
    slots, n_occ, n_aux, packed, mixed, coeff, near, far, wrapped,
    held, lent, stage, sent, came, far_sent, far_came, wrap_sems, local, stored,
):
    own = packed.shape[1]
    naux, nvir = stage.shape
    occ, aux = lax.axis_index("occ"), lax.axis_index("aux")
    mate = (lax.rem(occ + n_occ // 2, n_occ), aux)
    after = (lax.rem(occ + 1, n_occ), aux)
    before = (lax.rem(occ + n_occ - 1, n_occ), aux)
    peers = [(occ, peer_of(aux, s, n_aux)) for s in range(n_aux)]

    barrier = pltpu.get_barrier_semaphore()
    greeted = [mate, after, before] + peers[1:]
    for device in greeted:
        pl.semaphore_signal(barrier, inc=1, device_id=device, device_id_type=MESH)
    pl.semaphore_wait(barrier, len(greeted))

    wrap = pltpu.make_async_remote_copy(
        packed.at[n_aux - 1], wrapped, wrap_sems.at[0], wrap_sems.at[1], device_id=after, device_id_type=MESH
    )
    wrap.start()

    def piece(kind, land, source, t, s):
        if s == 0:
            return pltpu.make_async_copy(source, land.at[t, 0], local.at[kind, t])
        return pltpu.make_async_remote_copy(
            source, land.at[t, s], sent.at[kind, t, s], came.at[kind, t, s], device_id=peers[s], device_id_type=MESH
        )

    def send_own(t, carry):
        for s in range(n_aux):
            piece(0, held, packed.at[peers[s][1], t], t, s).start()
        return carry

    def send_near(t, carry):
        for s in range(n_aux):
            to = peers[s][1]

            @pl.when(to == 0)
            def _():
                piece(1, lent, wrapped.at[t], t, s).start()

            @pl.when(to != 0)
            def _():
                piece(1, lent, packed.at[jnp.maximum(to - 1, 0), t], t, s).start()

        return carry

    def transform(kind, land, target, t):
        for s in range(n_aux):
            move = piece(kind, land, packed.at[0, 0], t, s)
            move.wait() if s == 0 else move.wait_recv()
        tile = 256

        def rows(i, carry):
            at = pl.ds(pl.multiple_of(i * tile, tile), tile)
            block = land[t].reshape(naux, nvir)
            stage[at, :] = jnp.dot(mixed[at, :], block, preferred_element_type=jnp.float32).astype(stage.dtype)
            return carry

        lax.fori_loop(0, naux // tile, rows, 0)
        out = pltpu.make_async_copy(stage, target.at[t], stored)
        out.start()
        out.wait()

    def far_copy(t):
        return pltpu.make_async_remote_copy(
            coeff.at[t], far.at[t], far_sent.at[t], far_came.at[t], device_id=mate, device_id_type=MESH
        )

    def own_slot(t, carry):
        transform(0, held, coeff, t)

        @pl.when(t < slots)
        def _():
            far_copy(t).start()

        return carry

    def near_slot(t, carry):
        transform(1, lent, near, t)
        return carry

    lax.fori_loop(0, own, send_own, 0)
    early = min(own, 2)
    lax.fori_loop(0, early, own_slot, 0)
    wrap.wait()
    lax.fori_loop(0, own, send_near, 0)
    lax.fori_loop(early, own, own_slot, 0)
    lax.fori_loop(0, own, near_slot, 0)

    def drain(t, carry):
        for kind, land in ((0, held), (1, lent)):
            for s in range(1, n_aux):
                piece(kind, land, packed.at[0, 0], t, s).wait_send()
        return carry

    lax.fori_loop(0, own, drain, 0)

    def finish(t, carry):
        far_copy(t).wait()
        return carry

    lax.fori_loop(0, slots, finish, 0)


def moved(packed, mixed, slots, n_occ, n_aux):
    _, own, depth, nvir = packed.shape
    naux = depth * n_aux
    anywhere = pl.BlockSpec(memory_space=pl.ANY)
    kind = packed.dtype
    dma = pltpu.SemaphoreType.DMA
    return pl.pallas_call(
        functools.partial(move_kernel, slots, n_occ, n_aux),
        out_shape=[
            jax.ShapeDtypeStruct((own, naux, nvir), kind),
            jax.ShapeDtypeStruct((own, naux, nvir), kind),
            jax.ShapeDtypeStruct((slots, naux, nvir), kind),
            jax.ShapeDtypeStruct((own, depth, nvir), kind),
        ],
        in_specs=[anywhere, pl.BlockSpec(memory_space=pltpu.VMEM)],
        out_specs=[anywhere] * 4,
        scratch_shapes=[
            pltpu.VMEM((own, n_aux, depth, nvir), kind),
            pltpu.VMEM((own, n_aux, depth, nvir), kind),
            pltpu.VMEM((naux, nvir), kind),
            dma((2, own, n_aux)),
            dma((2, own, n_aux)),
            dma((slots,)),
            dma((slots,)),
            dma((2,)),
            dma((2, own)),
            dma(()),
        ],
        compiler_params=pltpu.CompilerParams(
            collective_id=slots, has_side_effects=True, vmem_limit_bytes=60 * 1024 * 1024
        ),
    )(packed, mixed)


def on_device(integrals, metric, e_occ, e_vir, partner, screen):
    n_occ, n_aux = lax.axis_size("occ"), lax.axis_size("aux")
    groups = n_occ * n_aux
    depth, held, nvir = integrals.shape
    own = held // n_aux
    naux = depth * n_aux
    occ, aux = lax.axis_index("occ"), lax.axis_index("aux")
    device = occ * n_aux + aux
    shifts = (1, groups // 2)

    code = (partner * 2 + screen).reshape(1, own * ROUNDS)
    code = jnp.pad(code, ((0, 7), (0, 128 - own * ROUNDS)))
    table = everyones(code, n_occ, n_aux)[:, 0, : own * ROUNDS].reshape(groups, own, ROUNDS)
    place = jnp.arange(own, dtype=jnp.int32)
    wanted = (table[:, :, 1, None] // 2 == place) & (table[:, :, 1, None] % 2 == 1)
    wanted = jnp.roll(jnp.any(wanted, axis=1), -shifts[1], axis=0)
    count = jnp.sum(wanted, axis=1, dtype=jnp.int32)
    first = jnp.cumsum(wanted, axis=1, dtype=jnp.int32) - 1
    last = count[:, None] + jnp.cumsum(~wanted, axis=1, dtype=jnp.int32) - 1
    rank = jnp.where(wanted, first, last)
    order = jnp.sum(jnp.where(rank[:, None, :] == place[None, :, None], place[None, None, :], 0), axis=2)

    here = lax.dynamic_slice(order, (occ * n_aux, 0), (n_aux, own)) + own * jnp.arange(n_aux, dtype=jnp.int32)[:, None]
    packed = jnp.transpose(integrals, (1, 0, 2)).at[here.reshape(-1)].get(mode="promise_in_bounds")
    packed = packed.reshape(n_aux, own, depth, nvir)
    mixed = metric.reshape(naux, n_aux, depth)
    mixed = jnp.concatenate(
        [lax.dynamic_index_in_dim(mixed, peer_of(aux, s, n_aux), 1, False) for s in range(n_aux)], axis=1
    )

    e_own = lax.dynamic_slice(e_occ, (device * own,), (own,))
    at, e_right = [], []
    for rnd in range(ROUNDS):
        source = (device - shifts[rnd]) % groups
        e_right.append(e_occ.at[source * own + partner[:, rnd]].get(mode="promise_in_bounds"))
        ranks = lax.dynamic_index_in_dim(rank, source, 0, False)
        at.append(ranks.at[partner[:, rnd]].get(mode="promise_in_bounds"))
    mine = lax.dynamic_index_in_dim(rank, device, 0, False)

    def run(slots):
        coeff, near, far, _ = moved(packed, mixed, slots, n_occ, n_aux)
        at1 = jnp.minimum(at[1], slots - 1)
        density = jnp.zeros((nvir, nvir), jnp.float32)
        amp0, density = amplitudes(coeff, near, mine, at[0], screen[:, 0], e_own, e_right[0], e_vir, density)
        amp1, density = amplitudes(coeff, far, mine, at1, screen[:, 1], e_own, e_right[1], e_vir, density)
        gamma = gradient(near, far, amp0, amp1, at[0], at1, screen[:, 0], screen[:, 1])
        return gamma, density

    gamma, density = run(own)
    rows = density.reshape(n_occ, n_aux, nvir // groups, nvir)
    rows = lax.psum_scatter(rows, "aux", scatter_dimension=1, tiled=False)
    rows = lax.psum_scatter(rows, "occ", scatter_dimension=0, tiled=False)
    block = lax.all_gather(rows, "aux", axis=0, tiled=True)
    return gamma, block / NOCC


def solution(mesh):
    return jax.shard_map(
        on_device,
        mesh=mesh,
        in_specs=(P("aux", "occ", None), P(), P(), P(), P(BOTH, None), P(BOTH, None)),
        out_specs=(P(None, BOTH, None), P("occ", None)),
        check_vma=False,
    )
```

```python
import functools

import jax
import jax.numpy as jnp
from jax import lax
from jax.experimental import pallas as pl
from jax.experimental.pallas import tpu as pltpu
from jax.sharding import PartitionSpec as P

NOCC = 256
ROUNDS = 2
BOTH = ("occ", "aux")
NT = (((1,), (1,)), ((), ()))
TN = (((0,), (0,)), ((), ()))

MESH = pl.DeviceIdType.MESH


def amp_kernel(left_at, right_at, kept, e_left, e_right, left, right, col, row, before, amp, density):
    pair = pl.program_id(0)

    @pl.when(pair == 0)
    def _():
        density[...] = before[...]

    @pl.when(kept[pair] != 0)
    def _():
        both = lax.dot_general(left[0], right[0], TN, preferred_element_type=jnp.float32)
        gap = col[...] + row[...] - e_left[pair] - e_right[pair]
        block = (both / gap).astype(jnp.bfloat16)
        amp[0] = block
        density[...] += lax.dot_general(block, block, NT, preferred_element_type=jnp.float32)

    @pl.when(kept[pair] == 0)
    def _():
        amp[0] = jnp.zeros_like(amp[0])


def amplitudes(left, right, left_at, right_at, kept, e_left, e_right, e_vir, before):
    _, naux, nvir = left.shape
    pairs = left_at.shape[0]
    wide = (1, naux, nvir)
    return pl.pallas_call(
        amp_kernel,
        grid_spec=pltpu.PrefetchScalarGridSpec(
            num_scalar_prefetch=5,
            grid=(pairs,),
            in_specs=[
                pl.BlockSpec(wide, lambda m, li, ri, *_: (li[m], 0, 0)),
                pl.BlockSpec(wide, lambda m, li, ri, *_: (ri[m], 0, 0)),
                pl.BlockSpec((nvir, 1), lambda m, *_: (0, 0)),
                pl.BlockSpec((1, nvir), lambda m, *_: (0, 0)),
                pl.BlockSpec((nvir, nvir), lambda m, *_: (0, 0)),
            ],
            out_specs=[
                pl.BlockSpec((1, nvir, nvir), lambda m, *_: (m, 0, 0)),
                pl.BlockSpec((nvir, nvir), lambda m, *_: (0, 0)),
            ],
        ),
        out_shape=[
            jax.ShapeDtypeStruct((pairs, nvir, nvir), jnp.bfloat16),
            jax.ShapeDtypeStruct((nvir, nvir), jnp.float32),
        ],
        cost_estimate=pl.CostEstimate(
            flops=2 * pairs * (naux + nvir) * nvir * nvir,
            bytes_accessed=4 * pairs * naux * nvir,
            transcendentals=0,
        ),
    )(left_at, right_at, kept, e_left, e_right, left, right, e_vir[:, None], e_vir[None, :], before)


def gamma_kernel(own, at0, at1, kept0, kept1, right0, right1, amp0, amp1, out, rows):
    for i in range(own):
        first, second = kept0[i] != 0, kept1[i] != 0

        def term0():
            return lax.dot_general(right0[at0[i]], amp0[i], NT, preferred_element_type=jnp.float32)

        def term1():
            return lax.dot_general(right1[at1[i]], amp1[i], NT, preferred_element_type=jnp.float32)

        @pl.when(first & second)
        def _():
            rows[i] = (term0() + term1()).astype(rows.dtype)

        @pl.when(first & jnp.logical_not(second))
        def _():
            rows[i] = term0().astype(rows.dtype)

        @pl.when(jnp.logical_not(first) & second)
        def _():
            rows[i] = term1().astype(rows.dtype)

        @pl.when(jnp.logical_not(first | second))
        def _():
            rows[i] = jnp.zeros_like(rows[i])

    out[...] = pltpu.einshape("ipa->pia", rows[...])


def gradient(right0, right1, amp0, amp1, at0, at1, kept0, kept1):
    own = amp0.shape[0]
    _, naux, nvir = right0.shape
    tile = min(256, naux)
    full = lambda p, *_: (0, 0, 0)
    return pl.pallas_call(
        functools.partial(gamma_kernel, own),
        grid_spec=pltpu.PrefetchScalarGridSpec(
            num_scalar_prefetch=4,
            grid=(naux // tile,),
            in_specs=[
                pl.BlockSpec((right0.shape[0], tile, nvir), lambda p, *_: (0, p, 0)),
                pl.BlockSpec((right1.shape[0], tile, nvir), lambda p, *_: (0, p, 0)),
                pl.BlockSpec(amp0.shape, full),
                pl.BlockSpec(amp1.shape, full),
            ],
            out_specs=pl.BlockSpec((tile, own, nvir), lambda p, *_: (p, 0, 0)),
            scratch_shapes=[pltpu.VMEM((own, tile, nvir), jnp.bfloat16)],
        ),
        out_shape=jax.ShapeDtypeStruct((naux, own, nvir), jnp.bfloat16),
        cost_estimate=pl.CostEstimate(
            flops=4 * own * naux * nvir * nvir, bytes_accessed=6 * own * naux * nvir, transcendentals=0
        ),
    )(at0, at1, kept0, kept1, right0, right1, amp0, amp1)


def table_kernel(n_occ, n_aux, row, table, send, recv, local):
    groups = n_occ * n_aux
    me = lax.axis_index("occ") * n_aux + lax.axis_index("aux")
    barrier = pltpu.get_barrier_semaphore()

    def place(step):
        other = lax.rem(me + step, groups)
        return (other // n_aux, lax.rem(other, n_aux))

    def greet(step, carry):
        pl.semaphore_signal(barrier, inc=1, device_id=place(step), device_id_type=MESH)
        return carry

    lax.fori_loop(1, groups, greet, 0)
    own = pltpu.make_async_copy(row, table.at[me], local)
    own.start()
    pl.semaphore_wait(barrier, groups - 1)

    def copy(step):
        return pltpu.make_async_remote_copy(
            row, table.at[me], send.at[step], recv.at[step], device_id=place(step), device_id_type=MESH
        )

    def start(step, carry):
        copy(step).start()
        return carry

    def finish(step, carry):
        came = lax.rem(me - step + groups, groups)
        pltpu.make_async_remote_copy(
            row, table.at[came], send.at[step], recv.at[step], device_id=place(step), device_id_type=MESH
        ).wait()
        return carry

    lax.fori_loop(1, groups, start, 0)
    own.wait()
    lax.fori_loop(1, groups, finish, 0)


def everyones(row, n_occ, n_aux):
    groups = n_occ * n_aux
    return pl.pallas_call(
        functools.partial(table_kernel, n_occ, n_aux),
        out_shape=jax.ShapeDtypeStruct((groups,) + row.shape, row.dtype),
        in_specs=[pl.BlockSpec(memory_space=pltpu.VMEM)],
        out_specs=pl.BlockSpec(memory_space=pltpu.VMEM),
        scratch_shapes=[
            pltpu.SemaphoreType.DMA((groups,)),
            pltpu.SemaphoreType.DMA((groups,)),
            pltpu.SemaphoreType.DMA(()),
        ],
        compiler_params=pltpu.CompilerParams(collective_id=0, has_side_effects=True),
    )(row)


def pack_kernel(order, x, out, turned):
    n_aux, own = out.shape[:2]
    turned[...] = pltpu.einshape("qja->jqa", x[...])
    for slot in range(n_aux * own):
        out[slot // own, slot % own] = turned[order[slot]]


def packed_blocks(x, order, n_aux):
    depth, held, nvir = x.shape
    own = held // n_aux
    tile = min(32, depth)
    return pl.pallas_call(
        pack_kernel,
        grid_spec=pltpu.PrefetchScalarGridSpec(
            num_scalar_prefetch=1,
            grid=(depth // tile,),
            in_specs=[pl.BlockSpec((tile, held, nvir), lambda q, *_: (q, 0, 0))],
            out_specs=pl.BlockSpec((n_aux, own, tile, nvir), lambda q, *_: (0, 0, q, 0)),
            scratch_shapes=[pltpu.VMEM((held, tile, nvir), x.dtype)],
        ),
        out_shape=jax.ShapeDtypeStruct((n_aux, own, depth, nvir), x.dtype),
    )(order, x)


def peer_of(i, step, n_aux):
    return i ^ step if n_aux & (n_aux - 1) == 0 else lax.rem(step + n_aux - i, n_aux)


def move_kernel(
    slots, n_occ, n_aux, packed, mixed, coeff, near, far, wrapped,
    held, lent, stage, sent, came, far_sent, far_came, wrap_sems, local, stored,
):
    own = packed.shape[1]
    naux, nvir = stage.shape
    occ, aux = lax.axis_index("occ"), lax.axis_index("aux")
    mate = (lax.rem(occ + n_occ // 2, n_occ), aux)
    after = (lax.rem(occ + 1, n_occ), aux)
    before = (lax.rem(occ + n_occ - 1, n_occ), aux)
    peers = [(occ, peer_of(aux, s, n_aux)) for s in range(n_aux)]

    barrier = pltpu.get_barrier_semaphore()
    greeted = [mate, after, before] + peers[1:]
    for device in greeted:
        pl.semaphore_signal(barrier, inc=1, device_id=device, device_id_type=MESH)
    pl.semaphore_wait(barrier, len(greeted))

    wrap = pltpu.make_async_remote_copy(
        packed.at[n_aux - 1], wrapped, wrap_sems.at[0], wrap_sems.at[1], device_id=after, device_id_type=MESH
    )
    wrap.start()

    def piece(kind, land, source, t, s):
        if s == 0:
            return pltpu.make_async_copy(source, land.at[t, aux], local.at[kind, t])
        return pltpu.make_async_remote_copy(
            source, land.at[t, aux], sent.at[kind, t, s], came.at[kind, t, s], device_id=peers[s], device_id_type=MESH
        )

    def send_own(t, carry):
        for s in range(n_aux):
            piece(0, held, packed.at[peers[s][1], t], t, s).start()
        return carry

    def send_near(t, carry):
        for s in range(n_aux):
            to = peers[s][1]

            @pl.when(to == 0)
            def _():
                piece(1, lent, wrapped.at[t], t, s).start()

            @pl.when(to != 0)
            def _():
                piece(1, lent, packed.at[jnp.maximum(to - 1, 0), t], t, s).start()

        return carry

    def transform(kind, land, target, t):
        for s in range(n_aux):
            if s == 0:
                piece(kind, land, packed.at[0, 0], t, 0).wait()
            else:
                pltpu.make_async_remote_copy(
                    packed.at[0, 0], land.at[t, peers[s][1]], sent.at[kind, t, s], came.at[kind, t, s],
                    device_id=peers[s], device_id_type=MESH,
                ).wait_recv()
        tile = 256

        def rows(i, carry):
            at = pl.ds(pl.multiple_of(i * tile, tile), tile)
            block = land[t].reshape(naux, nvir)
            stage[at, :] = jnp.dot(mixed[at, :], block, preferred_element_type=jnp.float32).astype(stage.dtype)
            return carry

        lax.fori_loop(0, naux // tile, rows, 0)
        out = pltpu.make_async_copy(stage, target.at[t], stored)
        out.start()
        out.wait()

    def far_copy(t):
        return pltpu.make_async_remote_copy(
            coeff.at[t], far.at[t], far_sent.at[t], far_came.at[t], device_id=mate, device_id_type=MESH
        )

    def own_slot(t, carry):
        transform(0, held, coeff, t)

        @pl.when(t < slots)
        def _():
            far_copy(t).start()

        return carry

    def near_slot(t, carry):
        transform(1, lent, near, t)
        return carry

    lax.fori_loop(0, own, send_own, 0)
    early = min(own, 2)
    lax.fori_loop(0, early, own_slot, 0)
    wrap.wait()
    lax.fori_loop(0, own, send_near, 0)
    lax.fori_loop(early, own, own_slot, 0)
    lax.fori_loop(0, own, near_slot, 0)

    def drain(t, carry):
        for kind, land in ((0, held), (1, lent)):
            for s in range(1, n_aux):
                piece(kind, land, packed.at[0, 0], t, s).wait_send()
        return carry

    lax.fori_loop(0, own, drain, 0)

    def finish(t, carry):
        far_copy(t).wait()
        return carry

    lax.fori_loop(0, slots, finish, 0)


def moved(packed, mixed, slots, n_occ, n_aux):
    _, own, depth, nvir = packed.shape
    naux = depth * n_aux
    anywhere = pl.BlockSpec(memory_space=pl.ANY)
    kind = packed.dtype
    dma = pltpu.SemaphoreType.DMA
    return pl.pallas_call(
        functools.partial(move_kernel, slots, n_occ, n_aux),
        out_shape=[
            jax.ShapeDtypeStruct((own, naux, nvir), kind),
            jax.ShapeDtypeStruct((own, naux, nvir), kind),
            jax.ShapeDtypeStruct((own, naux, nvir), kind),
            jax.ShapeDtypeStruct((own, depth, nvir), kind),
        ],
        in_specs=[anywhere, pl.BlockSpec(memory_space=pltpu.VMEM)],
        out_specs=[anywhere] * 4,
        scratch_shapes=[
            pltpu.VMEM((own, n_aux, depth, nvir), kind),
            pltpu.VMEM((own, n_aux, depth, nvir), kind),
            pltpu.VMEM((naux, nvir), kind),
            dma((2, own, n_aux)),
            dma((2, own, n_aux)),
            dma((slots,)),
            dma((slots,)),
            dma((2,)),
            dma((2, own)),
            dma(()),
        ],
        compiler_params=pltpu.CompilerParams(
            collective_id=slots, has_side_effects=True, vmem_limit_bytes=60 * 1024 * 1024
        ),
    )(packed, mixed)


def on_device(integrals, metric, e_occ, e_vir, partner, screen):
    n_occ, n_aux = lax.axis_size("occ"), lax.axis_size("aux")
    groups = n_occ * n_aux
    depth, held, nvir = integrals.shape
    own = held // n_aux
    naux = depth * n_aux
    occ, aux = lax.axis_index("occ"), lax.axis_index("aux")
    device = occ * n_aux + aux
    shifts = (1, groups // 2)

    code = (partner * 2 + screen).reshape(1, own * ROUNDS)
    code = jnp.pad(code, ((0, 7), (0, 128 - own * ROUNDS)))
    table = everyones(code, n_occ, n_aux)[:, 0, : own * ROUNDS].reshape(groups, own, ROUNDS)
    place = jnp.arange(own, dtype=jnp.int32)
    wanted = (table[:, :, 1, None] // 2 == place) & (table[:, :, 1, None] % 2 == 1)
    wanted = jnp.roll(jnp.any(wanted, axis=1), -shifts[1], axis=0)
    count = jnp.sum(wanted, axis=1, dtype=jnp.int32)
    first = jnp.cumsum(wanted, axis=1, dtype=jnp.int32) - 1
    last = count[:, None] + jnp.cumsum(~wanted, axis=1, dtype=jnp.int32) - 1
    rank = jnp.where(wanted, first, last)
    order = jnp.sum(jnp.where(rank[:, None, :] == place[None, :, None], place[None, None, :], 0), axis=2)

    here = lax.dynamic_slice(order, (occ * n_aux, 0), (n_aux, own)) + own * jnp.arange(n_aux, dtype=jnp.int32)[:, None]
    packed = packed_blocks(integrals, here.reshape(-1), n_aux)

    e_own = lax.dynamic_slice(e_occ, (device * own,), (own,))
    at, e_right = [], []
    for rnd in range(ROUNDS):
        source = (device - shifts[rnd]) % groups
        e_right.append(e_occ.at[source * own + partner[:, rnd]].get(mode="promise_in_bounds"))
        ranks = lax.dynamic_index_in_dim(rank, source, 0, False)
        at.append(ranks.at[partner[:, rnd]].get(mode="promise_in_bounds"))
    mine = lax.dynamic_index_in_dim(rank, device, 0, False)

    most = jnp.max(count)
    fewest = max(1, own - 4)
    choices = list(range(fewest, own + 1))
    branch = jnp.clip(most - fewest, 0, len(choices) - 1)
    coeff, near, far = lax.switch(
        branch, [lambda slots=slots: tuple(moved(packed, metric, slots, n_occ, n_aux)[:3]) for slots in choices]
    )
    kept = [screen[:, 0], screen[:, 1]]
    at1 = jnp.minimum(at[1], jnp.maximum(most, 1) - 1)
    density = jnp.zeros((nvir, nvir), jnp.float32)
    amp0, density = amplitudes(coeff, near, mine, at[0], kept[0], e_own, e_right[0], e_vir, density)
    amp1, density = amplitudes(coeff, far, mine, at1, kept[1], e_own, e_right[1], e_vir, density)
    gamma = gradient(near, far, amp0, amp1, at[0], at1, kept[0], kept[1])
    rows = density.reshape(n_occ, n_aux, nvir // groups, nvir)
    rows = lax.psum_scatter(rows, "aux", scatter_dimension=1, tiled=False)
    rows = lax.psum_scatter(rows, "occ", scatter_dimension=0, tiled=False)
    block = lax.all_gather(rows, "aux", axis=0, tiled=True)
    return gamma, block / NOCC


def solution(mesh):
    return jax.shard_map(
        on_device,
        mesh=mesh,
        in_specs=(P("aux", "occ", None), P(), P(), P(), P(BOTH, None), P(BOTH, None)),
        out_specs=(P(None, BOTH, None), P("occ", None)),
        check_vma=False,
    )
```

```python
import functools

import jax
import jax.numpy as jnp
from jax import lax
from jax.experimental import pallas as pl
from jax.experimental.pallas import tpu as pltpu
from jax.sharding import PartitionSpec as P

NOCC = 256
ROUNDS = 2
BOTH = ("occ", "aux")
NT = (((1,), (1,)), ((), ()))
TN = (((0,), (0,)), ((), ()))

MESH = pl.DeviceIdType.MESH


def amp_kernel(left_at, right_at, kept, e_left, e_right, left, right, col, row, before, amp, density):
    pair = pl.program_id(0)

    @pl.when(pair == 0)
    def _():
        density[...] = before[...]

    @pl.when(kept[pair] != 0)
    def _():
        both = lax.dot_general(left[0], right[0], TN, preferred_element_type=jnp.float32)
        gap = col[...] + row[...] - e_left[pair] - e_right[pair]
        block = (both / gap).astype(jnp.bfloat16)
        amp[0] = block
        density[...] += lax.dot_general(block, block, NT, preferred_element_type=jnp.float32)

    @pl.when(kept[pair] == 0)
    def _():
        amp[0] = jnp.zeros_like(amp[0])


def amplitudes(left, right, left_at, right_at, kept, e_left, e_right, e_vir, before):
    _, naux, nvir = left.shape
    pairs = left_at.shape[0]
    wide = (1, naux, nvir)
    return pl.pallas_call(
        amp_kernel,
        grid_spec=pltpu.PrefetchScalarGridSpec(
            num_scalar_prefetch=5,
            grid=(pairs,),
            in_specs=[
                pl.BlockSpec(wide, lambda m, li, ri, *_: (li[m], 0, 0)),
                pl.BlockSpec(wide, lambda m, li, ri, *_: (ri[m], 0, 0)),
                pl.BlockSpec((nvir, 1), lambda m, *_: (0, 0)),
                pl.BlockSpec((1, nvir), lambda m, *_: (0, 0)),
                pl.BlockSpec((nvir, nvir), lambda m, *_: (0, 0)),
            ],
            out_specs=[
                pl.BlockSpec((1, nvir, nvir), lambda m, *_: (m, 0, 0)),
                pl.BlockSpec((nvir, nvir), lambda m, *_: (0, 0)),
            ],
        ),
        out_shape=[
            jax.ShapeDtypeStruct((pairs, nvir, nvir), jnp.bfloat16),
            jax.ShapeDtypeStruct((nvir, nvir), jnp.float32),
        ],
        cost_estimate=pl.CostEstimate(
            flops=2 * pairs * (naux + nvir) * nvir * nvir,
            bytes_accessed=4 * pairs * naux * nvir,
            transcendentals=0,
        ),
    )(left_at, right_at, kept, e_left, e_right, left, right, e_vir[:, None], e_vir[None, :], before)


def gamma_kernel(own, at0, at1, kept0, kept1, right0, right1, amp0, amp1, out, rows):
    def orbital(i, carry):
        first, second = kept0[i] != 0, kept1[i] != 0

        def term0():
            return lax.dot_general(right0[at0[i]], amp0[i], NT, preferred_element_type=jnp.float32)

        def term1():
            return lax.dot_general(right1[at1[i]], amp1[i], NT, preferred_element_type=jnp.float32)

        @pl.when(first & second)
        def _():
            rows[i] = (term0() + term1()).astype(rows.dtype)

        @pl.when(first & jnp.logical_not(second))
        def _():
            rows[i] = term0().astype(rows.dtype)

        @pl.when(jnp.logical_not(first) & second)
        def _():
            rows[i] = term1().astype(rows.dtype)

        @pl.when(jnp.logical_not(first | second))
        def _():
            rows[i] = jnp.zeros_like(rows[i])

        return carry

    lax.fori_loop(0, own, orbital, 0)
    out[...] = pltpu.einshape("ipa->pia", rows[...])


def gradient(right0, right1, amp0, amp1, at0, at1, kept0, kept1, half, before=None):
    own = amp0.shape[0]
    _, naux, nvir = right0.shape
    tile = min(512, naux // 2)
    tiles = naux // 2 // tile
    skip = half * tiles
    full = lambda p, *_: (0, 0, 0)
    first = before is None
    body = functools.partial(gamma_kernel, own)

    def onto(*refs):
        body(*refs[:8], *refs[9:])

    return pl.pallas_call(
        body if first else onto,
        grid_spec=pltpu.PrefetchScalarGridSpec(
            num_scalar_prefetch=4,
            grid=(tiles,),
            in_specs=[
                pl.BlockSpec((right0.shape[0], tile, nvir), lambda p, *_: (0, p + skip, 0)),
                pl.BlockSpec((right1.shape[0], tile, nvir), lambda p, *_: (0, p + skip, 0)),
                pl.BlockSpec(amp0.shape, full),
                pl.BlockSpec(amp1.shape, full),
            ]
            + ([] if first else [pl.BlockSpec(memory_space=pl.ANY)]),
            out_specs=pl.BlockSpec((tile, own, nvir), lambda p, *_: (p + skip, 0, 0)),
            scratch_shapes=[pltpu.VMEM((own, tile, nvir), jnp.bfloat16)],
        ),
        out_shape=jax.ShapeDtypeStruct((naux, own, nvir), jnp.bfloat16),
        input_output_aliases={} if first else {8: 0},
        cost_estimate=pl.CostEstimate(
            flops=2 * own * naux * nvir * nvir, bytes_accessed=3 * own * naux * nvir, transcendentals=0
        ),
    )(at0, at1, kept0, kept1, right0, right1, amp0, amp1, *(() if first else (before,)))


def table_kernel(n_occ, n_aux, row, table, send, recv, local):
    groups = n_occ * n_aux
    me = lax.axis_index("occ") * n_aux + lax.axis_index("aux")
    barrier = pltpu.get_barrier_semaphore()

    def place(step):
        other = lax.rem(me + step, groups)
        return (other // n_aux, lax.rem(other, n_aux))

    def greet(step, carry):
        pl.semaphore_signal(barrier, inc=1, device_id=place(step), device_id_type=MESH)
        return carry

    lax.fori_loop(1, groups, greet, 0)
    own = pltpu.make_async_copy(row, table.at[me], local)
    own.start()
    pl.semaphore_wait(barrier, groups - 1)

    def copy(step):
        return pltpu.make_async_remote_copy(
            row, table.at[me], send.at[step], recv.at[step], device_id=place(step), device_id_type=MESH
        )

    def start(step, carry):
        copy(step).start()
        return carry

    def finish(step, carry):
        came = lax.rem(me - step + groups, groups)
        pltpu.make_async_remote_copy(
            row, table.at[came], send.at[step], recv.at[step], device_id=place(step), device_id_type=MESH
        ).wait()
        return carry

    lax.fori_loop(1, groups, start, 0)
    own.wait()
    lax.fori_loop(1, groups, finish, 0)


def everyones(row, n_occ, n_aux):
    groups = n_occ * n_aux
    return pl.pallas_call(
        functools.partial(table_kernel, n_occ, n_aux),
        out_shape=jax.ShapeDtypeStruct((groups,) + row.shape, row.dtype),
        in_specs=[pl.BlockSpec(memory_space=pltpu.VMEM)],
        out_specs=pl.BlockSpec(memory_space=pltpu.VMEM),
        scratch_shapes=[
            pltpu.SemaphoreType.DMA((groups,)),
            pltpu.SemaphoreType.DMA((groups,)),
            pltpu.SemaphoreType.DMA(()),
        ],
        compiler_params=pltpu.CompilerParams(collective_id=0, has_side_effects=True),
    )(row)


def pack_kernel(base, table, x, out, turned):
    n_aux, own = out.shape[:2]
    turned[...] = pltpu.einshape("qja->jqa", x[...])
    for slot in range(n_aux * own):
        reader = base[0] + slot // own
        out[slot // own, slot % own] = turned[slot // own * own + table[reader, own + slot % own]]


def packed_blocks(x, base, table, n_aux):
    depth, held, nvir = x.shape
    own = held // n_aux
    tile = min(32, depth)
    return pl.pallas_call(
        pack_kernel,
        grid_spec=pltpu.PrefetchScalarGridSpec(
            num_scalar_prefetch=2,
            grid=(depth // tile,),
            in_specs=[pl.BlockSpec((tile, held, nvir), lambda q, *_: (q, 0, 0))],
            out_specs=pl.BlockSpec((n_aux, own, tile, nvir), lambda q, *_: (0, 0, q, 0)),
            scratch_shapes=[pltpu.VMEM((held, tile, nvir), x.dtype)],
        ),
        out_shape=jax.ShapeDtypeStruct((n_aux, own, depth, nvir), x.dtype),
    )(base, table, x)


def peer_of(i, step, n_aux):
    return i ^ step if n_aux & (n_aux - 1) == 0 else lax.rem(step + n_aux - i, n_aux)


def shares(total, own, core):
    caps = ((total + 1) // 2, total // 2)
    spill = tuple(min(own - caps[1 - c], caps[c]) for c in range(2))
    pick = lambda pair: pair[0] + core * (pair[1] - pair[0])
    return pick(caps), pick(caps[::-1]), pick(spill), pick(spill[::-1])


def move_kernel(
    total, n_occ, n_aux, at_left, at_right, fill_from, kept, e_left, e_right,
    packed, mixed, col, row, coeff, near, far, wrapped, fills, amp, density,
    pool, lent, stage, sent, came, far_sent, far_came, side_sent, side_came, cross_sent, cross_came,
    wrap_sems, local, stored,
):
    own, depth = packed.shape[1:3]
    naux, nvir = stage.shape
    occ, aux = lax.axis_index("occ"), lax.axis_index("aux")
    core = lax.rem(occ, 2)
    cap, cap_mate, spill, spill_mate = shares(total, own, core)
    most_spill = fills.shape[0]
    mate = (lax.rem(occ + n_occ // 2, n_occ), aux)
    after = (lax.rem(occ + 1, n_occ), aux)
    before = (lax.rem(occ + n_occ - 1, n_occ), aux)
    side = (occ + 1 - 2 * core, aux)
    peers = [(occ, peer_of(aux, s, n_aux)) for s in range(n_aux)]

    barrier = pltpu.get_barrier_semaphore()
    greeted = [mate, after, before, side] + peers[1:]
    for device in greeted:
        pl.semaphore_signal(barrier, inc=1, device_id=device, device_id_type=MESH)
    pl.semaphore_wait(barrier, len(greeted))

    def remote(source, target, send, recv, device):
        return pltpu.make_async_remote_copy(source, target, send, recv, device_id=device, device_id_type=MESH)

    wrap = remote(packed.at[n_aux - 1], wrapped, wrap_sems.at[0], wrap_sems.at[1], after)
    wrap.start()

    def part(land, t, q):
        return land.at[t, pl.ds(pl.multiple_of(q * depth, depth), depth)]

    def piece(kind, land, source, t, s, q):
        if s == 0:
            return pltpu.make_async_copy(source, part(land, t, q), local.at[kind, t])
        return remote(source, part(land, t, q), sent.at[kind, t, s], came.at[kind, t, s], peers[s])

    def send_own(t, carry):
        for s in range(n_aux):
            piece(0, pool, packed.at[peers[s][1], t], t, s, aux).start()
        return carry

    def send_near(t, carry):
        for s in range(n_aux):
            to = peers[s][1]

            @pl.when(to == 0)
            def _():
                piece(1, lent, wrapped.at[t], t, s, aux).start()

            @pl.when(to != 0)
            def _():
                piece(1, lent, packed.at[jnp.maximum(to - 1, 0), t], t, s, aux).start()

        return carry

    tile = min(256, naux)

    def transform(kind, land, target, t):
        for s in range(n_aux):
            move = piece(kind, land, packed.at[0, 0], t, s, peers[s][1])
            move.wait() if s == 0 else move.wait_recv()

        def rows(i, carry):
            at = pl.ds(pl.multiple_of(i * tile, tile), tile)
            stage[at, :] = jnp.dot(mixed[at, :], land[t], preferred_element_type=jnp.float32).astype(stage.dtype)
            return carry

        def back(i, carry):
            at = pl.ds(pl.multiple_of(i * tile, tile), tile)
            land[t, at, :] = stage[at, :]
            return carry

        lax.fori_loop(0, naux // tile, rows, 0)
        lax.fori_loop(0, naux // tile, back, 0)
        out = pltpu.make_async_copy(land.at[t], target.at[t], stored)
        out.start()
        out.wait()

    def far_copy(source, t):
        return remote(source, far.at[t], far_sent.at[t], far_came.at[t], mate)

    def side_copy(t, x):
        return remote(coeff.at[t], pool.at[own + x], side_sent.at[x], side_came.at[x], side)

    def cross_copy(t, f, place):
        return remote(far.at[t], far.at[place + f], cross_sent.at[f], cross_came.at[f], side)

    def own_slot(t, carry):
        transform(0, pool, coeff, t)

        @pl.when(t < cap - spill)
        def _():
            far_copy(coeff.at[t], t).start()

        @pl.when((t >= cap) & (t < cap + spill_mate))
        def _():
            side_copy(t, jnp.maximum(t - cap, 0)).start()

        return carry

    def near_slot(t, carry):
        transform(1, lent, near, t)
        return carry

    lax.fori_loop(0, own, send_own, 0)
    early = min(own, 2)
    lax.fori_loop(0, early, own_slot, 0)
    wrap.wait()
    lax.fori_loop(0, own, send_near, 0)
    lax.fori_loop(early, own, own_slot, 0)

    def side_wait(x, carry):
        side_copy(0, x).wait_recv()
        return carry

    lax.fori_loop(0, spill, side_wait, 0)

    def fill(f, carry):
        def copy(i, inner):
            at = pl.ds(pl.multiple_of(i * tile, tile), tile)
            stage[at, :] = pool[fill_from[f], at, :]
            return inner

        lax.fori_loop(0, naux // tile, copy, 0)
        out = pltpu.make_async_copy(stage, fills.at[f], stored)
        out.start()
        out.wait()
        far_copy(fills.at[f], cap - spill + f).start()
        return carry

    lax.fori_loop(0, spill, fill, 0)
    lax.fori_loop(0, own, near_slot, 0)

    density[...] = jnp.zeros_like(density)

    def pair(i, carry):
        both = lax.dot_general(pool[at_left[i]], lent[at_right[i]], TN, preferred_element_type=jnp.float32)
        gap = col[...] + row[...] - e_left[i] - e_right[i]
        block = (kept[i] * both / gap).astype(amp.dtype)
        amp[i] = block
        density[...] += lax.dot_general(block, block, NT, preferred_element_type=jnp.float32)
        return carry

    lax.fori_loop(0, own, pair, 0)

    def drain(t, carry):
        for kind, land in ((0, pool), (1, lent)):
            for s in range(1, n_aux):
                piece(kind, land, packed.at[0, 0], t, s, aux).wait_send()
        return carry

    def side_drain(x, carry):
        side_copy(0, x).wait_send()
        return carry

    def direct(t, carry):
        far_copy(coeff.at[t], t).wait()
        return carry

    def mirror(f, carry):
        t = cap - spill + f
        far_copy(fills.at[f], t).wait()
        cross_copy(t, f, cap_mate).start()
        return carry

    def cross_drain(f, carry):
        cross_copy(0, f, cap_mate).wait_send()
        return carry

    def cross_wait(f, carry):
        cross_copy(0, f, cap).wait_recv()
        return carry

    lax.fori_loop(0, own, drain, 0)
    lax.fori_loop(0, spill_mate, side_drain, 0)
    lax.fori_loop(0, cap - spill, direct, 0)
    lax.fori_loop(0, spill, mirror, 0)
    lax.fori_loop(0, spill, cross_drain, 0)
    lax.fori_loop(0, spill_mate, cross_wait, 0)


def moved(packed, mixed, e_vir, numbers, total, n_occ, n_aux):
    _, own, depth, nvir = packed.shape
    naux = depth * n_aux
    spill = max(1, *(shares(total, own, core)[2] for core in range(2)))
    anywhere = pl.BlockSpec(memory_space=pl.ANY)
    fast = pl.BlockSpec(memory_space=pltpu.VMEM)
    kind = packed.dtype
    dma = pltpu.SemaphoreType.DMA
    wide = lambda count: jax.ShapeDtypeStruct((count, naux, nvir), kind)
    return pl.pallas_call(
        functools.partial(move_kernel, total, n_occ, n_aux),
        out_shape=[
            wide(own),
            wide(own),
            wide(own),
            jax.ShapeDtypeStruct((own, depth, nvir), kind),
            wide(spill),
            jax.ShapeDtypeStruct((own, nvir, nvir), kind),
            jax.ShapeDtypeStruct((nvir, nvir), jnp.float32),
        ],
        in_specs=[pl.BlockSpec(memory_space=pltpu.SMEM)] * len(numbers) + [anywhere, fast, fast, fast],
        out_specs=[anywhere] * 5 + [fast] * 2,
        scratch_shapes=[
            pltpu.VMEM((own + spill, naux, nvir), kind),
            pltpu.VMEM((own, naux, nvir), kind),
            pltpu.VMEM((naux, nvir), kind),
            dma((2, own, n_aux)),
            dma((2, own, n_aux)),
            dma((own,)),
            dma((own,)),
            dma((spill,)),
            dma((spill,)),
            dma((spill,)),
            dma((spill,)),
            dma((2,)),
            dma((2, own)),
            dma(()),
        ],
        compiler_params=pltpu.CompilerParams(
            collective_id=total, has_side_effects=True, vmem_limit_bytes=63 * 1024 * 1024
        ),
    )(*numbers, packed, mixed, e_vir[:, None], e_vir[None, :])


def on_device(integrals, metric, e_occ, e_vir, partner, screen):
    n_occ, n_aux = lax.axis_size("occ"), lax.axis_size("aux")
    groups = n_occ * n_aux
    depth, held, nvir = integrals.shape
    own = held // n_aux
    naux = depth * n_aux
    occ, aux = lax.axis_index("occ"), lax.axis_index("aux")
    device = occ * n_aux + aux
    shifts = (1, groups // 2)

    place = jnp.arange(own, dtype=jnp.int32)
    kept = [screen[:, 0], screen[:, 1]]
    wanted = jnp.any((partner[:, 1, None] == place) & (kept[1][:, None] != 0), axis=0)
    below = place[None, :] < place[:, None]
    count = jnp.sum(wanted, dtype=jnp.int32)
    first = jnp.sum(below & wanted[None, :], axis=1, dtype=jnp.int32)
    rank = jnp.where(wanted, first, count + place - first)
    order = jnp.sum(jnp.where(rank[None, :] == place[:, None], place[None, :], 0), axis=1)
    lines = jnp.concatenate([rank, order, count[None]])[None]
    lines = jnp.pad(lines, ((0, 7), (0, 128 - 2 * own - 1)))
    table = everyones(lines, n_occ, n_aux)[:, 0, :]

    reader = ((occ + n_occ // 2) % n_occ) * n_aux
    packed = packed_blocks(integrals, reader[None], table, n_aux)

    counts = table[:, 2 * own].reshape(n_occ // 2, 2, n_aux)
    choices = sorted(set(range(own + 2, 2 * own - 2)) | {2 * own})
    branch = jnp.sum(jnp.max(jnp.sum(counts, axis=1)) > jnp.array(choices[:-1], jnp.int32), dtype=jnp.int32)
    total = jnp.array(choices, jnp.int32)[branch]
    core = occ % 2
    caps = jnp.stack([(total + 1) // 2, total // 2])
    cap, cap_mate = caps[core], caps[1 - core]
    spill, spill_mate = jnp.minimum(own - cap_mate, cap), jnp.minimum(own - cap, cap_mate)

    def ranking(source):
        return lax.dynamic_index_in_dim(table, (source + shifts[1]) % groups, 0, False)

    e_own = lax.dynamic_slice(e_occ, (device * own,), (own,))
    at, e_right = [], []
    for rnd in range(ROUNDS):
        source = (device - shifts[rnd]) % groups
        e_right.append(e_occ.at[source * own + partner[:, rnd]].get(mode="promise_in_bounds"))
        at.append(ranking(source).at[partner[:, rnd]].get(mode="promise_in_bounds"))
    mine = ranking(device)[:own]
    beyond = cap + spill_mate - 1 - (at[1] - cap)
    at1 = jnp.clip(jnp.where(at[1] < cap, at[1], beyond), 0, own - 1)
    side_count = ranking((occ + 1 - 2 * core) * n_aux + aux)[2 * own]
    step = spill - 1 - place
    fill_from = jnp.where(step < side_count - cap_mate, own + step, cap - spill + place)
    fill_from = jnp.clip(fill_from, 0, own + jnp.maximum(spill, 1) - 1)
    numbers = (mine, at[0], fill_from, kept[0].astype(jnp.float32), e_own, e_right[0])

    def chosen(total):
        coeff, near, far, _, _, amp, density = moved(packed, metric, e_vir, numbers, total, n_occ, n_aux)
        return coeff, near, far, amp, density

    coeff, near, far, amp0, density = lax.switch(
        branch,
        [
            functools.partial(chosen, total) for total in choices
        ],
    )
    amp1, density = amplitudes(coeff, far, mine, at1, kept[1], e_own, e_right[1], e_vir, density)
    rows = density.reshape(n_occ, n_aux, nvir // groups, nvir)
    rows = lax.psum_scatter(rows, "aux", scatter_dimension=1, tiled=False)
    gamma = gradient(near, far, amp0, amp1, at[0], at1, kept[0], kept[1], 0)
    rows, amp1 = lax.optimization_barrier((rows, amp1))
    rows = lax.psum_scatter(rows, "occ", scatter_dimension=0, tiled=False)
    gamma = gradient(near, far, amp0, amp1, at[0], at1, kept[0], kept[1], 1, gamma)
    block = lax.all_gather(rows, "aux", axis=0, tiled=True)
    return gamma, block / NOCC


def solution(mesh):
    return jax.shard_map(
        on_device,
        mesh=mesh,
        in_specs=(P("aux", "occ", None), P(), P(), P(), P(BOTH, None), P(BOTH, None)),
        out_specs=(P(None, BOTH, None), P("occ", None)),
        check_vma=False,
    )
```

```python
import functools

import jax
import jax.numpy as jnp
from jax import lax
from jax.experimental import pallas as pl
from jax.experimental.pallas import tpu as pltpu
from jax.sharding import PartitionSpec as P

NOCC = 256
ROUNDS = 2
BOTH = ("occ", "aux")
NT = (((1,), (1,)), ((), ()))
TN = (((0,), (0,)), ((), ()))

MESH = pl.DeviceIdType.MESH


def gamma_kernel(own, at, right, amp, begun, out, rows):
    now = lax.rem(pl.program_id(0), 2)
    for i in range(own):
        term = lax.dot_general(right[at[1, i]], amp[at[3, i]], NT, preferred_element_type=jnp.float32)
        rows[now, i] = (begun[i] + term).astype(rows.dtype)
    out[...] = pltpu.einshape("ipa->pia", rows[1 - now])


def gradient(right, amp, begun, ints):
    own, naux, nvir = right.shape
    tile = min(256, naux)
    tiles = naux // tile
    this = lambda p, *_: (0, jnp.minimum(p, tiles - 1), 0)
    return pl.pallas_call(
        functools.partial(gamma_kernel, own),
        grid_spec=pltpu.PrefetchScalarGridSpec(
            num_scalar_prefetch=1,
            grid=(tiles + 1,),
            in_specs=[
                pl.BlockSpec((own, tile, nvir), this),
                pl.BlockSpec(amp.shape, lambda p, *_: (0, 0, 0)),
                pl.BlockSpec((own, tile, nvir), this),
            ],
            out_specs=pl.BlockSpec((tile, own, nvir), lambda p, *_: (jnp.maximum(p - 1, 0), 0, 0)),
            scratch_shapes=[pltpu.VMEM((2, own, tile, nvir), jnp.bfloat16)],
        ),
        out_shape=jax.ShapeDtypeStruct((naux, own, nvir), jnp.bfloat16),
    )(ints, right, amp, begun)


def table_kernel(n_occ, n_aux, row, table, send, recv, local):
    groups = n_occ * n_aux
    me = lax.axis_index("occ") * n_aux + lax.axis_index("aux")
    barrier = pltpu.get_barrier_semaphore()

    def place(step):
        other = lax.rem(me + step, groups)
        return (other // n_aux, lax.rem(other, n_aux))

    def greet(step, carry):
        pl.semaphore_signal(barrier, inc=1, device_id=place(step), device_id_type=MESH)
        return carry

    lax.fori_loop(1, groups, greet, 0)
    own = pltpu.make_async_copy(row, table.at[me], local)
    own.start()
    pl.semaphore_wait(barrier, groups - 1)

    def copy(step):
        return pltpu.make_async_remote_copy(
            row, table.at[me], send.at[step], recv.at[step], device_id=place(step), device_id_type=MESH
        )

    def start(step, carry):
        copy(step).start()
        return carry

    def finish(step, carry):
        came = lax.rem(me - step + groups, groups)
        pltpu.make_async_remote_copy(
            row, table.at[came], send.at[step], recv.at[step], device_id=place(step), device_id_type=MESH
        ).wait()
        return carry

    lax.fori_loop(1, groups, start, 0)
    own.wait()
    lax.fori_loop(1, groups, finish, 0)


def everyones(row, n_occ, n_aux):
    groups = n_occ * n_aux
    return pl.pallas_call(
        functools.partial(table_kernel, n_occ, n_aux),
        out_shape=jax.ShapeDtypeStruct((groups,) + row.shape, row.dtype),
        in_specs=[pl.BlockSpec(memory_space=pltpu.VMEM)],
        out_specs=pl.BlockSpec(memory_space=pltpu.VMEM),
        scratch_shapes=[
            pltpu.SemaphoreType.DMA((groups,)),
            pltpu.SemaphoreType.DMA((groups,)),
            pltpu.SemaphoreType.DMA(()),
        ],
        compiler_params=pltpu.CompilerParams(collective_id=0, has_side_effects=True),
    )(row)


def pack_kernel(base, table, x, out, turned):
    n_aux, own = out.shape[:2]
    turned[...] = pltpu.einshape("qja->jqa", x[...])
    for slot in range(n_aux * own):
        reader = base[0] + slot // own
        out[slot // own, slot % own] = turned[slot // own * own + table[reader, own + slot % own]]


def packed_blocks(x, base, table, n_aux):
    depth, held, nvir = x.shape
    own = held // n_aux
    tile = min(32, depth)
    return pl.pallas_call(
        pack_kernel,
        grid_spec=pltpu.PrefetchScalarGridSpec(
            num_scalar_prefetch=2,
            grid=(depth // tile,),
            in_specs=[pl.BlockSpec((tile, held, nvir), lambda q, *_: (q, 0, 0))],
            out_specs=pl.BlockSpec((n_aux, own, tile, nvir), lambda q, *_: (0, 0, q, 0)),
            scratch_shapes=[pltpu.VMEM((held, tile, nvir), x.dtype)],
        ),
        out_shape=jax.ShapeDtypeStruct((n_aux, own, depth, nvir), x.dtype),
    )(base, table, x)


def peer_of(i, step, n_aux):
    return i ^ step if n_aux & (n_aux - 1) == 0 else lax.rem(step + n_aux - i, n_aux)


def shares(total, own, core):
    caps = ((total + 1) // 2, total // 2)
    spill = tuple(min(own - caps[1 - c], caps[c]) for c in range(2))
    pick = lambda pair: pair[0] + core * (pair[1] - pair[0])
    return pick(caps), pick(caps[::-1]), pick(spill), pick(spill[::-1])


def move_kernel(
    total, n_occ, n_aux, ints, floats, packed, mixed, col, row,
    far, begun, coeff, wrapped, fills, amp, block_out,
    pool, lent, stage, term, kept_amp, parts, half, sum1, from_side, from_aux, from_z, gathered,
    sent, came, far_sent, far_came, side_sent, side_came, cross_sent, cross_came,
    wrap_sems, local, stored, fold_sent, fold_came,
):
    own, depth = packed.shape[1:3]
    naux, nvir = stage.shape
    occ, aux = lax.axis_index("occ"), lax.axis_index("aux")
    core = lax.rem(occ, 2)
    cap, cap_mate, spill, spill_mate = shares(total, own, core)
    most_z = n_occ // 2
    mate = (lax.rem(occ + n_occ // 2, n_occ), aux)
    after = (lax.rem(occ + 1, n_occ), aux)
    before = (lax.rem(occ + n_occ - 1, n_occ), aux)
    side = (occ + 1 - 2 * core, aux)
    peers = [(occ, peer_of(aux, s, n_aux)) for s in range(n_aux)]
    column = [(lax.rem(occ + 2 * k, n_occ), aux) for k in range(most_z)]
    column_before = [(lax.rem(occ + n_occ - 2 * k, n_occ), aux) for k in range(most_z)]

    barrier = pltpu.get_barrier_semaphore()
    greeted = [after, before, side] + peers[1:] + column[1:]
    for device in greeted:
        pl.semaphore_signal(barrier, inc=1, device_id=device, device_id_type=MESH)
    pl.semaphore_wait(barrier, len(greeted))

    def remote(source, target, send, recv, device):
        return pltpu.make_async_remote_copy(source, target, send, recv, device_id=device, device_id_type=MESH)

    wrap = remote(packed.at[n_aux - 1], wrapped, wrap_sems.at[0], wrap_sems.at[1], after)
    wrap.start()

    def part(land, t, q):
        return land.at[t, pl.ds(pl.multiple_of(q * depth, depth), depth)]

    def piece(kind, land, source, t, s, q):
        if s == 0:
            return pltpu.make_async_copy(source, part(land, t, q), local.at[kind, t])
        return remote(source, part(land, t, q), sent.at[kind, t, s], came.at[kind, t, s], peers[s])

    def send_own(t, carry):
        for s in range(n_aux):
            piece(0, pool, packed.at[peers[s][1], t], t, s, aux).start()
        return carry

    def send_near(t, carry):
        for s in range(n_aux):
            to = peers[s][1]

            @pl.when(to == 0)
            def _():
                piece(1, lent, wrapped.at[t], t, s, aux).start()

            @pl.when(to != 0)
            def _():
                piece(1, lent, packed.at[jnp.maximum(to - 1, 0), t], t, s, aux).start()

        return carry

    tile = min(256, naux)

    def put(source, target):
        out = pltpu.make_async_copy(source, target, stored)
        out.start()
        out.wait()

    def transform(kind, land, t):
        for s in range(n_aux):
            move = piece(kind, land, packed.at[0, 0], t, s, peers[s][1])
            move.wait() if s == 0 else move.wait_recv()

        def rows(i, carry):
            at = pl.ds(pl.multiple_of(i * tile, tile), tile)
            stage[at, :] = jnp.dot(mixed[at, :], land[t], preferred_element_type=jnp.float32).astype(stage.dtype)
            return carry

        def back(i, carry):
            at = pl.ds(pl.multiple_of(i * tile, tile), tile)
            land[t, at, :] = stage[at, :]
            return carry

        lax.fori_loop(0, naux // tile, rows, 0)
        lax.fori_loop(0, naux // tile, back, 0)

    def far_copy(source, t):
        return remote(source, far.at[t], far_sent.at[t], far_came.at[t], mate)

    def side_copy(t, x):
        return remote(coeff.at[t], pool.at[own + x], side_sent.at[x], side_came.at[x], side)

    def cross_copy(t, f, place):
        return remote(far.at[t], far.at[place + f], cross_sent.at[f], cross_came.at[f], side)

    def own_slot(t, carry):
        @pl.when(t == min(own - 1, 2))
        def _():
            wrap.wait()
            lax.fori_loop(0, own, send_near, 0)

        transform(0, pool, t)
        put(pool.at[t], coeff.at[t])

        @pl.when(t < cap - spill)
        def _():
            far_copy(coeff.at[t], t).start()

        @pl.when((t >= cap) & (t < cap + spill_mate))
        def _():
            side_copy(t, jnp.maximum(t - cap, 0)).start()

        return carry

    def near_slot(t, carry):
        transform(1, lent, t)
        return carry

    lax.fori_loop(0, own, send_own, 0)
    lax.fori_loop(0, own, own_slot, 0)

    def side_wait(x, carry):
        side_copy(0, x).wait_recv()
        return carry

    lax.fori_loop(0, spill, side_wait, 0)

    def fill(f, carry):
        def copy(i, inner):
            at = pl.ds(pl.multiple_of(i * tile, tile), tile)
            stage[at, :] = pool[ints[2, f], at, :]
            return inner

        lax.fori_loop(0, naux // tile, copy, 0)
        put(stage, fills.at[f])
        far_copy(fills.at[f], cap - spill + f).start()
        return carry

    lax.fori_loop(0, spill, fill, 0)
    lax.fori_loop(0, own, near_slot, 0)

    parts[...] = jnp.zeros_like(parts)

    def amplitude(left, right, kept, gap):
        both = lax.dot_general(left, right, TN, preferred_element_type=jnp.float32)
        block = (kept * both / (col[...] + row[...] - gap[0] - gap[1])).astype(amp.dtype)
        square = lax.dot_general(block, block, NT, preferred_element_type=jnp.float32)
        parts[...] += square.reshape(parts.shape)
        return block

    def pair0(i, carry):
        kept_amp[...] = amplitude(pool[ints[4, i]], lent[ints[0, i]], floats[0, i], (floats[2, i], floats[4, i]))

        def rows(k, inner):
            at = pl.ds(pl.multiple_of(k * tile, tile), tile)
            term[at, :] = lax.dot_general(
                lent[ints[0, i], at, :], kept_amp[...], NT, preferred_element_type=jnp.float32
            )
            return inner

        lax.fori_loop(0, naux // tile, rows, 0)
        put(term, begun.at[i])
        return carry

    lax.fori_loop(0, own, pair0, 0)

    def pair1(m):
        amp[m] = amplitude(pool[ints[5, m]], lent[ints[6, m]], floats[1, m], (floats[3, m], floats[5, m]))

    def crossed(f, carry):
        cross_copy(0, f, cap).wait_recv()
        put(far.at[cap + f], lent.at[cap + f])
        return carry

    def next_pair(m, carry):
        @pl.when(m < cap)
        def _():
            far_copy(coeff.at[m], m).wait_recv()

            @pl.when(m >= cap - spill)
            def _():
                cross_copy(m, jnp.maximum(m - (cap - spill), 0), cap_mate).start()

            put(far.at[m], lent.at[m])

        @pl.when(m == cap)
        def _():
            lax.fori_loop(0, spill_mate, crossed, 0)

        pair1(m)
        return carry

    lax.fori_loop(0, own, next_pair, 0)

    fold = lambda k, source, target, device: remote(source, target, fold_sent.at[k], fold_came.at[k], device)
    swap = fold(0, parts.at[:, 1 - core], from_side, side)
    swap.start()
    swap.wait()
    half[...] = parts[:, core] + from_side[...]
    moves = [fold(s, half.at[:, peers[s][1]], from_aux.at[s - 1], peers[s]) for s in range(1, n_aux)]
    for move in moves:
        move.start()
    for move in moves:
        move.wait()
    sum1[...] = half[:, aux] + jnp.sum(from_aux[...], axis=0)
    moves = []
    for k in range(1, most_z):
        moves.append(fold(n_aux + k - 1, sum1.at[column[k][0] // 2], from_z.at[k - 1], column[k]))
    for move in moves:
        move.start()
    for move in moves:
        move.wait()
    gathered[aux] = (sum1[occ // 2] + jnp.sum(from_z[...], axis=0)) / NOCC
    base = n_aux + most_z - 2
    moves = [fold(base + s, gathered.at[aux], gathered.at[aux], peers[s]) for s in range(1, n_aux)]
    for move in moves:
        move.start()
    for s, move in enumerate(moves):
        move.wait_send()
        fold(base + s + 1, gathered.at[aux], gathered.at[peers[s + 1][1]], peers[s + 1]).wait_recv()
    block_out[...] = gathered[...].reshape(block_out.shape)

    def drain(t, carry):
        for kind, land in ((0, pool), (1, lent)):
            for s in range(1, n_aux):
                piece(kind, land, packed.at[0, 0], t, s, aux).wait_send()
        return carry

    def side_drain(x, carry):
        side_copy(0, x).wait_send()
        return carry

    def far_drain(t, carry):
        far_copy(coeff.at[t], t).wait_send()
        return carry

    def cross_drain(f, carry):
        cross_copy(0, f, cap_mate).wait_send()
        return carry

    lax.fori_loop(0, own, drain, 0)
    lax.fori_loop(0, spill_mate, side_drain, 0)
    lax.fori_loop(0, cap, far_drain, 0)
    lax.fori_loop(0, spill, cross_drain, 0)


def moved(packed, mixed, e_vir, ints, floats, total, n_occ, n_aux):
    _, own, depth, nvir = packed.shape
    naux = depth * n_aux
    spill = max(1, *(shares(total, own, core)[2] for core in range(2)))
    anywhere = pl.BlockSpec(memory_space=pl.ANY)
    fast = pl.BlockSpec(memory_space=pltpu.VMEM)
    scalars = pl.BlockSpec(memory_space=pltpu.SMEM)
    kind = packed.dtype
    dma = pltpu.SemaphoreType.DMA
    wide = lambda count: jax.ShapeDtypeStruct((count, naux, nvir), kind)
    most_z, thin = n_occ // 2, nvir // (n_occ * n_aux)
    single = lambda *lead: pltpu.VMEM(lead + (thin, nvir), jnp.float32)
    folds = 2 * n_aux + most_z - 1
    return pl.pallas_call(
        functools.partial(move_kernel, total, n_occ, n_aux),
        out_shape=[
            wide(own),
            jax.ShapeDtypeStruct((own, naux, nvir), jnp.float32),
            wide(own),
            jax.ShapeDtypeStruct((own, depth, nvir), kind),
            wide(spill),
            jax.ShapeDtypeStruct((own, nvir, nvir), kind),
            jax.ShapeDtypeStruct((nvir // n_occ, nvir), jnp.float32),
        ],
        in_specs=[scalars] * 2 + [anywhere, fast, fast, fast],
        out_specs=[anywhere] * 5 + [fast] * 2,
        scratch_shapes=[
            pltpu.VMEM((own + spill, naux, nvir), kind),
            pltpu.VMEM((own, naux, nvir), kind),
            pltpu.VMEM((naux, nvir), kind),
            pltpu.VMEM((naux, nvir), jnp.float32),
            pltpu.VMEM((nvir, nvir), kind),
            single(most_z, 2, n_aux),
            single(most_z, n_aux),
            single(most_z),
            single(most_z, n_aux),
            single(n_aux - 1, most_z),
            single(most_z - 1),
            single(n_aux),
            dma((2, own, n_aux)),
            dma((2, own, n_aux)),
            dma((own,)),
            dma((own,)),
            dma((spill,)),
            dma((spill,)),
            dma((spill,)),
            dma((spill,)),
            dma((2,)),
            dma((2, own)),
            dma(()),
            dma((folds,)),
            dma((folds,)),
        ],
        compiler_params=pltpu.CompilerParams(
            collective_id=total, has_side_effects=True, vmem_limit_bytes=67043328
        ),
    )(ints, floats, packed, mixed, e_vir[:, None], e_vir[None, :])


def plan_kernel(choices, n_occ, n_aux, table, partner, screen, e_occ, ints, floats, branch):
    groups = n_occ * n_aux
    own = partner.shape[0]
    occ, aux = lax.axis_index("occ"), lax.axis_index("aux")
    device = occ * n_aux + aux
    far_by = groups // 2
    reader = lambda source: lax.rem(source + far_by, groups)
    count = lambda source: table[reader(source), 2 * own]

    def chip(c, most):
        source = c // n_aux * 2 * n_aux + lax.rem(c, n_aux)
        return jnp.maximum(most, count(source) + count(source + n_aux))

    most = lax.fori_loop(0, groups // 2, chip, 0)
    chosen, total = 0, choices[0]
    for k in range(1, len(choices)):
        over = most > choices[k - 1]
        chosen = jnp.where(over, k, chosen)
        total = jnp.where(over, choices[k], total)
    branch[0] = jnp.int32(chosen)
    core = lax.rem(occ, 2)
    caps = ((total + 1) // 2, total // 2)
    cap, cap_mate = jnp.where(core == 0, caps[0], caps[1]), jnp.where(core == 0, caps[1], caps[0])
    spill, spill_mate = jnp.minimum(own - cap_mate, cap), jnp.minimum(own - cap, cap_mate)
    side_count = count((occ + 1 - 2 * core) * n_aux + aux)
    near, far = lax.rem(device + groups - 1, groups), lax.rem(device + groups - far_by, groups)
    ranks = [table[reader(far), partner[i, 1]] for i in range(own)]
    keys = [jnp.where(screen[i, 1] != 0, ranks[i], own) for i in range(own)]
    for i in range(own):
        ints[0, i] = table[reader(near), partner[i, 0]]
        beyond = cap + spill_mate - 1 - (ranks[i] - cap)
        slot = jnp.clip(jnp.where(ranks[i] < cap, ranks[i], beyond), 0, own - 1)
        ints[1, i] = slot
        step = spill - 1 - i
        fill = jnp.where(step < side_count - cap_mate, own + step, cap - spill + i)
        ints[2, i] = jnp.clip(fill, 0, own - 1 + jnp.maximum(spill, 1))
        where = jnp.int32(0)
        for other in range(own):
            if other != i:
                ahead = keys[other] < keys[i] if other > i else keys[other] <= keys[i]
                where = where + jnp.where(ahead, 1, 0)
        ints[3, i] = where
        mine = table[reader(device), i]
        ints[4, i] = mine
        ints[5, where] = mine
        ints[6, where] = slot
        floats[0, i] = screen[i, 0].astype(jnp.float32)
        floats[1, where] = screen[i, 1].astype(jnp.float32)
        energy = e_occ[device * own + i]
        floats[2, i] = energy
        floats[3, where] = energy
        floats[4, i] = e_occ[near * own + partner[i, 0]]
        floats[5, where] = e_occ[far * own + partner[i, 1]]


def plan(choices, table, partner, screen, e_occ, n_occ, n_aux):
    own = partner.shape[0]
    scalars = pl.BlockSpec(memory_space=pltpu.SMEM)
    return pl.pallas_call(
        functools.partial(plan_kernel, choices, n_occ, n_aux),
        out_shape=[
            jax.ShapeDtypeStruct((7, own), jnp.int32),
            jax.ShapeDtypeStruct((6, own), jnp.float32),
            jax.ShapeDtypeStruct((1,), jnp.int32),
        ],
        in_specs=[scalars] * 4,
        out_specs=[scalars] * 3,
    )(table, partner, screen, e_occ)


def on_device(integrals, metric, e_occ, e_vir, partner, screen):
    n_occ, n_aux = lax.axis_size("occ"), lax.axis_size("aux")
    groups = n_occ * n_aux
    depth, held, nvir = integrals.shape
    own = held // n_aux
    naux = depth * n_aux
    occ, aux = lax.axis_index("occ"), lax.axis_index("aux")
    device = occ * n_aux + aux

    place = jnp.arange(own, dtype=jnp.int32)
    wanted = jnp.any((partner[:, 1, None] == place) & (screen[:, 1, None] != 0), axis=0)
    below = place[None, :] < place[:, None]
    count = jnp.sum(wanted, dtype=jnp.int32)
    first = jnp.sum(below & wanted[None, :], axis=1, dtype=jnp.int32)
    rank = jnp.where(wanted, first, count + place - first)
    order = jnp.sum(jnp.where(rank[None, :] == place[:, None], place[None, :], 0), axis=1)
    lines = jnp.concatenate([rank, order, count[None]])[None]
    lines = jnp.pad(lines, ((0, 7), (0, 128 - 2 * own - 1)))
    table = everyones(lines, n_occ, n_aux)[:, 0, :]

    reader = ((occ + n_occ // 2) % n_occ) * n_aux
    packed = packed_blocks(integrals, reader[None], table, n_aux)

    choices = sorted(set(range(own + 2, 2 * own - 2)) | {2 * own})
    ints, floats, branch = plan(choices, table, partner, screen, e_occ, n_occ, n_aux)

    def chosen(total):
        far, begun, _, _, _, amp, block = moved(packed, metric, e_vir, ints, floats, total, n_occ, n_aux)
        return far, begun, amp, block

    far, begun, amp, block = lax.switch(branch[0], [functools.partial(chosen, total) for total in choices])
    return gradient(far, amp, begun, ints), block


def solution(mesh):
    return jax.shard_map(
        on_device,
        mesh=mesh,
        in_specs=(P("aux", "occ", None), P(), P(), P(), P(BOTH, None), P(BOTH, None)),
        out_specs=(P(None, BOTH, None), P("occ", None)),
        check_vma=False,
    )
```

```python
import functools

import jax
import jax.numpy as jnp
from jax import lax
from jax.experimental import pallas as pl
from jax.experimental.pallas import tpu as pltpu
from jax.sharding import PartitionSpec as P

NOCC = 256
ROUNDS = 2
BOTH = ("occ", "aux")
NT = (((1,), (1,)), ((), ()))
TN = (((0,), (0,)), ((), ()))

MESH = pl.DeviceIdType.MESH


def gamma_kernel(own, at, right, amp, begun, out, rows):
    now = lax.rem(pl.program_id(0), 2)
    for i in range(own):
        term = lax.dot_general(right[at[1, i]], amp[at[3, i]], NT, preferred_element_type=jnp.float32)
        rows[now, i] = (begun[i] + term).astype(rows.dtype)
    out[...] = pltpu.einshape("ipa->pia", rows[1 - now])


def gradient(right, amp, begun, ints):
    slots, naux, nvir = right.shape
    own = amp.shape[0]
    tile = min(256, naux)
    tiles = naux // tile
    this = lambda p, *_: (0, jnp.minimum(p, tiles - 1), 0)
    return pl.pallas_call(
        functools.partial(gamma_kernel, own),
        grid_spec=pltpu.PrefetchScalarGridSpec(
            num_scalar_prefetch=1,
            grid=(tiles + 1,),
            in_specs=[
                pl.BlockSpec((slots, tile, nvir), this),
                pl.BlockSpec(amp.shape, lambda p, *_: (0, 0, 0)),
                pl.BlockSpec((own, tile, nvir), this),
            ],
            out_specs=pl.BlockSpec((tile, own, nvir), lambda p, *_: (jnp.maximum(p - 1, 0), 0, 0)),
            scratch_shapes=[pltpu.VMEM((2, own, tile, nvir), jnp.bfloat16)],
        ),
        out_shape=jax.ShapeDtypeStruct((naux, own, nvir), jnp.bfloat16),
    )(ints, right, amp, begun)


def table_kernel(n_occ, n_aux, partner, screen, table, row, send, recv, local):
    groups = n_occ * n_aux
    own = partner.shape[0]
    me = lax.axis_index("occ") * n_aux + lax.axis_index("aux")

    def wants(k):
        found = jnp.int32(0)
        for i in range(own):
            found = jnp.where((partner[i, 1] == k) & (screen[i, 1] != 0), 1, found)
        return found

    wanted = [wants(k) for k in range(own)]
    total = sum(wanted)
    lend = (total >= own // 2 + 1) & (total < own)
    ahead, slots = jnp.int32(0), []
    for k in range(own):
        behind = jnp.where(lend, total - 1, total) + k - ahead
        last = jnp.where(lend & (ahead == total - 1), own - 1, ahead)
        slots.append(jnp.where(wanted[k] == 1, last, behind))
        ahead = ahead + wanted[k]
    lane = lax.broadcasted_iota(jnp.int32, (1, 128), 1)
    line = jnp.where(lane == 2 * own, total, 0)
    for k in range(own):
        line = line + jnp.where(lane == k, slots[k], 0)
        turned = sum(jnp.where(slots[j] == k, j, 0) for j in range(own))
        line = line + jnp.where(lane == own + k, turned, 0)
    row[...] = line

    barrier = pltpu.get_barrier_semaphore()

    def place(step):
        other = lax.rem(me + step, groups)
        return (other // n_aux, lax.rem(other, n_aux))

    def greet(step, carry):
        pl.semaphore_signal(barrier, inc=1, device_id=place(step), device_id_type=MESH)
        return carry

    lax.fori_loop(1, groups, greet, 0)
    own_row = pltpu.make_async_copy(row, table.at[me], local)
    own_row.start()
    pl.semaphore_wait(barrier, groups - 1)

    def copy(step, came):
        return pltpu.make_async_remote_copy(
            row, table.at[came], send.at[step], recv.at[step], device_id=place(step), device_id_type=MESH
        )

    def start(step, carry):
        copy(step, me).start()
        return carry

    def finish(step, carry):
        copy(step, lax.rem(me - step + groups, groups)).wait()
        return carry

    lax.fori_loop(1, groups, start, 0)
    own_row.wait()
    lax.fori_loop(1, groups, finish, 0)


def rankings(partner, screen, n_occ, n_aux):
    groups = n_occ * n_aux
    scalars = pl.BlockSpec(memory_space=pltpu.SMEM)
    return pl.pallas_call(
        functools.partial(table_kernel, n_occ, n_aux),
        out_shape=jax.ShapeDtypeStruct((groups, 1, 128), jnp.int32),
        in_specs=[scalars] * 2,
        out_specs=pl.BlockSpec(memory_space=pltpu.VMEM),
        scratch_shapes=[
            pltpu.VMEM((1, 128), jnp.int32),
            pltpu.SemaphoreType.DMA((groups,)),
            pltpu.SemaphoreType.DMA((groups,)),
            pltpu.SemaphoreType.DMA(()),
        ],
        compiler_params=pltpu.CompilerParams(collective_id=0, has_side_effects=True),
    )(partner, screen)


def pack_kernel(base, table, x, out, turned):
    n_aux, own = out.shape[:2]
    turned[...] = pltpu.einshape("qja->jqa", x[...])
    for slot in range(n_aux * own):
        reader = base[0] + slot // own
        out[slot // own, slot % own] = turned[slot // own * own + table[reader, 0, own + slot % own]]


def packed_blocks(x, base, table, n_aux):
    depth, held, nvir = x.shape
    own = held // n_aux
    tile = min(32, depth)
    return pl.pallas_call(
        pack_kernel,
        grid_spec=pltpu.PrefetchScalarGridSpec(
            num_scalar_prefetch=2,
            grid=(depth // tile,),
            in_specs=[pl.BlockSpec((tile, held, nvir), lambda q, *_: (q, 0, 0))],
            out_specs=pl.BlockSpec((n_aux, own, tile, nvir), lambda q, *_: (0, 0, q, 0)),
            scratch_shapes=[pltpu.VMEM((held, tile, nvir), x.dtype)],
        ),
        out_shape=jax.ShapeDtypeStruct((n_aux, own, depth, nvir), x.dtype),
    )(base, table, x)


def peer_of(i, step, n_aux):
    return i ^ step if n_aux & (n_aux - 1) == 0 else lax.rem(step + n_aux - i, n_aux)


def shares(total, own):
    caps = ((total + 1) // 2, total // 2)
    spill = tuple(jnp.minimum(own - caps[1 - c], caps[c]) for c in range(2))
    return caps, spill


def fixed_shares(total, own):
    caps = ((total + 1) // 2, total // 2)
    return caps, tuple(min(own - caps[1 - c], caps[c]) for c in range(2))


def move_kernel(
    total, n_occ, n_aux, ints, floats, packed, mixed, col, row,
    far, begun, coeff, wrapped, fills, amp, block_out,
    pool, lent, stage, term, kept_amp, parts, half, sum1, from_side, from_aux, from_z, gathered,
    sent, came, far_sent, far_came, side_sent, side_came, cross_sent, cross_came,
    wrap_sems, local, stored, fold_sent, fold_came, lend_sent, lend_came,
):
    own, depth = packed.shape[1:3]
    naux, nvir = stage.shape
    occ, aux = lax.axis_index("occ"), lax.axis_index("aux")
    core = lax.rem(occ, 2)
    pick = lambda pair: pair[0] + core * (pair[1] - pair[0])
    caps, spills = fixed_shares(total, own)
    cap, cap_mate, spill, spill_mate = pick(caps), pick(caps[::-1]), pick(spills), pick(spills[::-1])
    pooled = total < 2 * own
    aside = own - min(caps) + 1 if pooled else 0
    most_z = n_occ // 2
    mate = (lax.rem(occ + n_occ // 2, n_occ), aux)
    after = (lax.rem(occ + 1, n_occ), aux)
    before = (lax.rem(occ + n_occ - 1, n_occ), aux)
    side = (occ + 1 - 2 * core, aux)
    above = (occ + 2 - 4 * lax.rem(occ // 2, 2), aux)
    peers = [(occ, peer_of(aux, s, n_aux)) for s in range(n_aux)]
    column = [(lax.rem(occ + 2 * k, n_occ), aux) for k in range(most_z)]
    column_before = [(lax.rem(occ + n_occ - 2 * k, n_occ), aux) for k in range(most_z)]

    barrier = pltpu.get_barrier_semaphore()
    greeted = [after, before, side] + peers[1:] + column[1:]
    for device in greeted:
        pl.semaphore_signal(barrier, inc=1, device_id=device, device_id_type=MESH)
    pl.semaphore_wait(barrier, len(greeted))

    def remote(source, target, send, recv, device):
        return pltpu.make_async_remote_copy(source, target, send, recv, device_id=device, device_id_type=MESH)

    wrap = remote(packed.at[n_aux - 1], wrapped, wrap_sems.at[0], wrap_sems.at[1], after)
    wrap.start()

    def part(land, t, q):
        return land.at[t, pl.ds(pl.multiple_of(q * depth, depth), depth)]

    def piece(kind, land, source, t, s, q):
        if s == 0:
            return pltpu.make_async_copy(source, part(land, t, q), local.at[kind, t])
        return remote(source, part(land, t, q), sent.at[kind, t, s], came.at[kind, t, s], peers[s])

    def send_own(step, carry):
        t = lax.rem(step + own - 1, own) if pooled else step
        for s in range(n_aux):
            piece(0, pool, packed.at[peers[s][1], t], t, s, aux).start()
        return carry

    def send_near(t, carry):
        for s in range(n_aux):
            to = peers[s][1]

            @pl.when(to == 0)
            def _():
                piece(1, lent, wrapped.at[t], t, s, aux).start()

            @pl.when(to != 0)
            def _():
                piece(1, lent, packed.at[jnp.maximum(to - 1, 0), t], t, s, aux).start()

        return carry

    tile = min(256, naux)

    def put(source, target):
        out = pltpu.make_async_copy(source, target, stored)
        out.start()
        out.wait()

    def transform(kind, land, t):
        for s in range(n_aux):
            move = piece(kind, land, packed.at[0, 0], t, s, peers[s][1])
            move.wait() if s == 0 else move.wait_recv()

        def rows(i, carry):
            at = pl.ds(pl.multiple_of(i * tile, tile), tile)
            stage[at, :] = jnp.dot(mixed[at, :], land[t], preferred_element_type=jnp.float32).astype(stage.dtype)
            return carry

        def back(i, carry):
            at = pl.ds(pl.multiple_of(i * tile, tile), tile)
            land[t, at, :] = stage[at, :]
            return carry

        lax.fori_loop(0, naux // tile, rows, 0)
        lax.fori_loop(0, naux // tile, back, 0)

    def far_copy(source, t):
        return remote(source, far.at[t], far_sent.at[t], far_came.at[t], mate)

    def side_copy(t, x):
        return remote(coeff.at[t], pool.at[own + x], side_sent.at[x], side_came.at[x], side)

    def cross_copy(t, f, place):
        return remote(far.at[t], far.at[place + f], cross_sent.at[f], cross_came.at[f], side)

    def lend_copy():
        return remote(coeff.at[own - 1], pool.at[own + aside], lend_sent.at[0], lend_came.at[0], above)

    def back_copy():
        return remote(far.at[cap - spill], far.at[own], lend_sent.at[1], lend_came.at[1], above)

    def own_slot(step, carry):
        t = lax.rem(step + own - 1, own) if pooled else step

        @pl.when(step == min(own - 1, 2))
        def _():
            wrap.wait()
            lax.fori_loop(0, own, send_near, 0)

        transform(0, pool, t)
        put(pool.at[t], coeff.at[t])

        @pl.when(t < cap - spill)
        def _():
            far_copy(coeff.at[t], t).start()

        if pooled:

            @pl.when(t >= cap - 1)
            def _():
                side_copy(t, jnp.maximum(t - (cap - 1), 0)).start()

            @pl.when(t == own - 1)
            def _():
                lend_copy().start()

        return carry

    def near_slot(t, carry):
        transform(1, lent, t)
        return carry

    lax.fori_loop(0, own, send_own, 0)
    lax.fori_loop(0, own, own_slot, 0)

    def side_wait(x, carry):
        side_copy(0, x).wait_recv()
        return carry

    if pooled:
        lax.fori_loop(0, own - cap_mate + 1, side_wait, 0)
        lend_copy().wait_recv()

    def fill(f, carry):
        def copy(i, inner):
            at = pl.ds(pl.multiple_of(i * tile, tile), tile)
            stage[at, :] = pool[ints[2, f], at, :]
            return inner

        lax.fori_loop(0, naux // tile, copy, 0)
        put(stage, fills.at[f])
        far_copy(fills.at[f], cap - spill + f).start()
        return carry

    lax.fori_loop(0, spill, fill, 0)
    lax.fori_loop(0, own, near_slot, 0)

    parts[...] = jnp.zeros_like(parts)

    def amplitude(left, right, kept, gap):
        both = lax.dot_general(left, right, TN, preferred_element_type=jnp.float32)
        block = (kept * both / (col[...] + row[...] - gap[0] - gap[1])).astype(amp.dtype)
        square = lax.dot_general(block, block, NT, preferred_element_type=jnp.float32)
        parts[...] += square.reshape(parts.shape)
        return block

    def pair0(i, carry):
        kept_amp[...] = amplitude(pool[ints[4, i]], lent[ints[0, i]], floats[0, i], (floats[2, i], floats[4, i]))

        def rows(k, inner):
            at = pl.ds(pl.multiple_of(k * tile, tile), tile)
            term[...] = lax.dot_general(
                lent[ints[0, i], at, :], kept_amp[...], NT, preferred_element_type=jnp.float32
            )
            put(term, begun.at[i, at])
            return inner

        lax.fori_loop(0, naux // tile, rows, 0)
        return carry

    lax.fori_loop(0, own, pair0, 0)

    def pair1(m, carry):
        kept_amp[...] = amplitude(pool[ints[5, m]], lent[ints[6, m]], floats[1, m], (floats[3, m], floats[5, m]))
        put(kept_amp, amp.at[m])
        return carry

    def arrive(u, carry):
        far_copy(coeff.at[u], u).wait_recv()
        if pooled:

            @pl.when(u == cap - spill)
            def _():
                back_copy().start()

            @pl.when(u >= cap - spill)
            def _():
                cross_copy(u, jnp.maximum(u - (cap - spill), 0), cap_mate).start()

        put(far.at[u], lent.at[u])
        if pooled:

            @pl.when(u >= 1)
            def _():
                pair1(jnp.maximum(u - 1, 0), 0)

        return carry

    def crossed(f, carry):
        cross_copy(0, f, cap).wait_recv()
        put(far.at[cap + f], lent.at[cap + f])
        return carry

    lax.fori_loop(0, cap, arrive, 0)
    if pooled:
        back_copy().wait_recv()
        put(far.at[own], lent.at[own])
        lax.fori_loop(0, spill_mate, crossed, 0)
    lax.fori_loop(cap - 1 if pooled else 0, own, pair1, 0)

    fold = lambda k, source, target, device: remote(source, target, fold_sent.at[k], fold_came.at[k], device)
    swap = fold(0, parts.at[:, 1 - core], from_side, side)
    swap.start()
    swap.wait()
    half[...] = parts[:, core] + from_side[...]
    moves = [fold(s, half.at[:, peers[s][1]], from_aux.at[s - 1], peers[s]) for s in range(1, n_aux)]
    for move in moves:
        move.start()
    for move in moves:
        move.wait()
    sum1[...] = half[:, aux] + jnp.sum(from_aux[...], axis=0)
    moves = []
    for k in range(1, most_z):
        moves.append(fold(n_aux + k - 1, sum1.at[column[k][0] // 2], from_z.at[k - 1], column[k]))
    for move in moves:
        move.start()
    for move in moves:
        move.wait()
    gathered[aux] = (sum1[occ // 2] + jnp.sum(from_z[...], axis=0)) / NOCC
    base = n_aux + most_z - 2
    moves = [fold(base + s, gathered.at[aux], gathered.at[aux], peers[s]) for s in range(1, n_aux)]
    for move in moves:
        move.start()
    for s, move in enumerate(moves):
        move.wait_send()
        fold(base + s + 1, gathered.at[aux], gathered.at[peers[s + 1][1]], peers[s + 1]).wait_recv()
    block_out[...] = gathered[...].reshape(block_out.shape)

    def drain(t, carry):
        for kind, land in ((0, pool), (1, lent)):
            for s in range(1, n_aux):
                piece(kind, land, packed.at[0, 0], t, s, aux).wait_send()
        return carry

    def side_drain(x, carry):
        side_copy(0, x).wait_send()
        return carry

    def far_drain(t, carry):
        far_copy(coeff.at[t], t).wait_send()
        return carry

    def cross_drain(f, carry):
        cross_copy(0, f, cap_mate).wait_send()
        return carry

    lax.fori_loop(0, own, drain, 0)
    lax.fori_loop(0, cap, far_drain, 0)
    if pooled:
        lax.fori_loop(0, own - cap + 1, side_drain, 0)
        lax.fori_loop(0, spill, cross_drain, 0)
        lend_copy().wait_send()
        back_copy().wait_send()


def moved(packed, mixed, e_vir, ints, floats, total, n_occ, n_aux):
    _, own, depth, nvir = packed.shape
    naux = depth * n_aux
    caps, spills = fixed_shares(total, own)
    spill, aside = max(1, *spills), own - min(caps) + 1 if total < 2 * own else 0
    anywhere = pl.BlockSpec(memory_space=pl.ANY)
    fast = pl.BlockSpec(memory_space=pltpu.VMEM)
    scalars = pl.BlockSpec(memory_space=pltpu.SMEM)
    kind = packed.dtype
    dma = pltpu.SemaphoreType.DMA
    wide = lambda count: jax.ShapeDtypeStruct((count, naux, nvir), kind)
    most_z, thin = n_occ // 2, nvir // (n_occ * n_aux)
    single = lambda *lead: pltpu.VMEM(lead + (thin, nvir), jnp.float32)
    folds = 2 * n_aux + most_z - 1
    return pl.pallas_call(
        functools.partial(move_kernel, total, n_occ, n_aux),
        out_shape=[
            wide(own + 1),
            jax.ShapeDtypeStruct((own, naux, nvir), jnp.float32),
            wide(own),
            jax.ShapeDtypeStruct((own, depth, nvir), kind),
            wide(spill),
            jax.ShapeDtypeStruct((own, nvir, nvir), kind),
            jax.ShapeDtypeStruct((nvir // n_occ, nvir), jnp.float32),
        ],
        in_specs=[scalars] * 2 + [anywhere, fast, fast, fast],
        out_specs=[anywhere] * 6 + [fast],
        scratch_shapes=[
            pltpu.VMEM((own + aside + 1, naux, nvir), kind),
            pltpu.VMEM((own + 1, naux, nvir), kind),
            pltpu.VMEM((naux, nvir), kind),
            pltpu.VMEM((min(256, naux), nvir), jnp.float32),
            pltpu.VMEM((nvir, nvir), kind),
            single(most_z, 2, n_aux),
            single(most_z, n_aux),
            single(most_z),
            single(most_z, n_aux),
            single(n_aux - 1, most_z),
            single(most_z - 1),
            single(n_aux),
            dma((2, own, n_aux)),
            dma((2, own, n_aux)),
            dma((own,)),
            dma((own,)),
            dma((max(1, aside),)),
            dma((max(1, aside),)),
            dma((spill,)),
            dma((spill,)),
            dma((2,)),
            dma((2, own)),
            dma(()),
            dma((folds,)),
            dma((folds,)),
            dma((2,)),
            dma((2,)),
        ],
        compiler_params=pltpu.CompilerParams(
            collective_id=total, has_side_effects=True, vmem_limit_bytes=67043328
        ),
    )(ints, floats, packed, mixed, e_vir[:, None], e_vir[None, :])


def lending(total, own, wanted):
    caps, spill = shares(total, own)
    over = [wanted[z][0] + wanted[z][1] - total for z in range(2)]
    flag = lambda test: jnp.where(test, 1, 0)
    lends = []
    for z in range(2):
        big = [wanted[z][c] > caps[c] for c in range(2)]
        one, two = over[z] == 1, over[z] == 2
        lends.append([flag((one & big[0]) | two), flag((one & jnp.logical_not(big[0])) | two)])
    fine, items, excess = True, [], []
    for z in range(2):
        fine = fine & (over[z] <= 2)
        for c in range(2):
            fine = fine & ((lends[z][c] == 0) | (wanted[z][c] > caps[c]))
        items.append(
            [lends[1 - z][c] + jnp.maximum(wanted[z][c] - caps[c] + spill[c], 0) - lends[z][c] for c in range(2)]
        )
        excess.append([jnp.maximum(items[z][c] - spill[c], 0) for c in range(2)])
        for c in range(2):
            fine = fine & (jnp.minimum(items[z][c], spill[c]) + excess[z][1 - c] <= spill[c])
            fine = fine & ((lends[z][0] + lends[z][1] == 0) | (lends[1 - z][c] == 0))
    return lends, items, excess, fine


def plan_kernel(choices, n_occ, n_aux, table, partner, screen, e_occ, ints, floats, branch):
    groups = n_occ * n_aux
    own = partner.shape[0]
    occ, aux = lax.axis_index("occ"), lax.axis_index("aux")
    device = occ * n_aux + aux
    far_by = groups // 2
    reader = lambda source: lax.rem(source + far_by, groups)
    slot_of = lambda source, orbital: table[reader(source), 0, orbital]

    def counts(first):
        count = lambda o: table[reader(o * n_aux + aux_of), 0, 2 * own]
        aux_of = lax.rem(first, n_aux)
        row = first // n_aux
        return [[count(row + 2 * z + c) for c in range(2)] for z in range(2)]

    chosen, total = jnp.int32(0), jnp.int32(choices[0])
    for k in range(1, len(choices)):

        def quad(q, good):
            first = q // n_aux * 4 * n_aux + lax.rem(q, n_aux)
            return good & jnp.where(lending(choices[k - 1], own, counts(first))[3], 1, 0)

        over = lax.fori_loop(0, groups // 4, quad, jnp.int32(1)) == 0
        still = over & (chosen == k - 1)
        chosen = jnp.where(still, k, chosen)
        total = jnp.where(still, choices[k], total)
    branch[0] = chosen
    pooled = total < 2 * own
    caps, spills = shares(total, own)
    core = lax.rem(occ, 2)
    level = lax.rem(occ // 2, 2)
    by_core = lambda pair, c: jnp.where(c == 0, pair[0], pair[1])
    at = lambda grid, z, c: by_core([by_core(grid[0], c), by_core(grid[1], c)], z)
    cap, cap_mate = by_core(caps, core), by_core(caps, 1 - core)
    spill, spill_mate = by_core(spills, core), by_core(spills, 1 - core)
    aside = own - caps[1] + 1
    many = own // 2 + 1

    def shared_slot(item, first_shared, wanted):
        lent = (wanted >= many) & (item == wanted - 1 - first_shared)
        return jnp.where(lent, own - 1, first_shared + item)

    wanted = counts((occ - 2 * level - core) * n_aux + aux)
    lends, items, excess, _ = lending(total, own, wanted)
    carries, mine, theirs = at(lends, 1 - level, core), at(items, level, core), at(excess, level, 1 - core)
    wanted_own, wanted_side = at(wanted, level, core), at(wanted, level, 1 - core)
    side_carries = at(lends, 1 - level, 1 - core)
    for f in range(own):
        own_item = shared_slot(f - carries, cap - spill, wanted_own)
        k = f - mine
        side_slot = shared_slot(spill_mate - side_carries + k, cap_mate - spill_mate, wanted_side)
        side_item = jnp.where(k < theirs, own + side_slot - (cap_mate - 1), 0)
        item = jnp.where(f < mine, own_item, side_item)
        item = jnp.where((f == 0) & (carries == 1), own + aside, item)
        ints[2, f] = jnp.where(pooled, jnp.clip(item, 0, own + aside), 0)

    near, far = lax.rem(device + groups - 1, groups), lax.rem(device + groups - far_by, groups)
    source_occ = far // n_aux
    wanted = counts((source_occ - 2 * level - core) * n_aux + aux)
    lends, items, _, _ = lending(total, own, wanted)
    lent_one, carries = at(lends, level, core), at(lends, 1 - level, core)
    wanted_own = at(wanted, level, core)
    side_items = jnp.minimum(at(items, level, 1 - core), spill_mate)

    def far_slot(slot):
        special = (slot == own - 1) & (wanted_own >= many)
        item = jnp.where(special, wanted_own - 1 - (cap - spill), slot - (cap - spill))
        f = carries + item
        shared = jnp.where(f < spill, cap - spill + f, cap + side_items + f - spill)
        place = jnp.where(special & (lent_one == 1), own, shared)
        place = jnp.where(slot < cap - spill, slot, place)
        return jnp.clip(place, 0, own)

    found = [far_slot(slot_of(far, partner[i, 1])) for i in range(own)]
    found = [jnp.where(screen[i, 1] != 0, found[i], 0) for i in range(own)]
    keys = [jnp.where(screen[i, 1] != 0, found[i], own + 1) for i in range(own)]
    for i in range(own):
        ints[0, i] = slot_of(near, partner[i, 0])
        ints[1, i] = found[i]
        where = jnp.int32(0)
        for other in range(own):
            if other != i:
                ahead = keys[other] < keys[i] if other > i else keys[other] <= keys[i]
                where = where + jnp.where(ahead, 1, 0)
        ints[3, i] = where
        mine = slot_of(device, i)
        ints[4, i] = mine
        ints[5, where] = mine
        ints[6, where] = found[i]
        floats[0, i] = screen[i, 0].astype(jnp.float32)
        floats[1, where] = screen[i, 1].astype(jnp.float32)
        energy = e_occ[device * own + i]
        floats[2, i] = energy
        floats[3, where] = energy
        floats[4, i] = e_occ[near * own + partner[i, 0]]
        floats[5, where] = e_occ[far * own + partner[i, 1]]


def plan(choices, table, partner, screen, e_occ, n_occ, n_aux):
    own = partner.shape[0]
    scalars = pl.BlockSpec(memory_space=pltpu.SMEM)
    return pl.pallas_call(
        functools.partial(plan_kernel, choices, n_occ, n_aux),
        out_shape=[
            jax.ShapeDtypeStruct((7, own), jnp.int32),
            jax.ShapeDtypeStruct((6, own), jnp.float32),
            jax.ShapeDtypeStruct((1,), jnp.int32),
        ],
        in_specs=[scalars] * 4,
        out_specs=[scalars] * 3,
    )(table, partner, screen, e_occ)


def on_device(integrals, metric, e_occ, e_vir, partner, screen):
    n_occ, n_aux = lax.axis_size("occ"), lax.axis_size("aux")
    groups = n_occ * n_aux
    depth, held, nvir = integrals.shape
    own = held // n_aux
    occ, aux = lax.axis_index("occ"), lax.axis_index("aux")
    device = occ * n_aux + aux

    table = rankings(partner, screen, n_occ, n_aux)

    reader = ((occ + n_occ // 2) % n_occ) * n_aux
    packed = packed_blocks(integrals, reader[None], table, n_aux)

    choices = sorted(set(range(own + 1, 2 * own - 3)) | {2 * own})
    ints, floats, branch = plan(choices, table, partner, screen, e_occ, n_occ, n_aux)

    def chosen(total):
        far, begun, _, _, _, amp, block = moved(packed, metric, e_vir, ints, floats, total, n_occ, n_aux)
        return far, begun, amp, block

    far, begun, amp, block = lax.switch(branch[0], [functools.partial(chosen, total) for total in choices])
    return gradient(far, amp, begun, ints), block


def solution(mesh):
    return jax.shard_map(
        on_device,
        mesh=mesh,
        in_specs=(P("aux", "occ", None), P(), P(), P(), P(BOTH, None), P(BOTH, None)),
        out_specs=(P(None, BOTH, None), P("occ", None)),
        check_vma=False,
    )
```

```python
import functools

import jax
import jax.numpy as jnp
from jax import lax
from jax.experimental import pallas as pl
from jax.experimental.pallas import tpu as pltpu
from jax.sharding import PartitionSpec as P

NOCC = 256
ROUNDS = 2
BOTH = ("occ", "aux")
NT = (((1,), (1,)), ((), ()))
TN = (((0,), (0,)), ((), ()))

MESH = pl.DeviceIdType.MESH


def gamma_kernel(own, at, right, amp, begun, out, rows):
    now = lax.rem(pl.program_id(0), 2)
    for i in range(own):
        term = lax.dot_general(right[at[1, i]], amp[at[3, i]], NT, preferred_element_type=jnp.float32)
        rows[now, i] = (begun[i] + term).astype(rows.dtype)
    out[...] = pltpu.einshape("ipa->pia", rows[1 - now])


def gradient(right, amp, begun, ints):
    slots, naux, nvir = right.shape
    own = amp.shape[0]
    tile = min(256, naux)
    tiles = naux // tile
    this = lambda p, *_: (0, jnp.minimum(p, tiles - 1), 0)
    return pl.pallas_call(
        functools.partial(gamma_kernel, own),
        grid_spec=pltpu.PrefetchScalarGridSpec(
            num_scalar_prefetch=1,
            grid=(tiles + 1,),
            in_specs=[
                pl.BlockSpec((slots, tile, nvir), this),
                pl.BlockSpec(amp.shape, lambda p, *_: (0, 0, 0)),
                pl.BlockSpec((own, tile, nvir), this),
            ],
            out_specs=pl.BlockSpec((tile, own, nvir), lambda p, *_: (jnp.maximum(p - 1, 0), 0, 0)),
            scratch_shapes=[pltpu.VMEM((2, own, tile, nvir), jnp.bfloat16)],
        ),
        out_shape=jax.ShapeDtypeStruct((naux, own, nvir), jnp.bfloat16),
    )(ints, right, amp, begun)


def table_kernel(n_occ, n_aux, partner, screen, table, row, send, recv, local):
    groups = n_occ * n_aux
    own = partner.shape[0]
    me = lax.axis_index("occ") * n_aux + lax.axis_index("aux")

    def wants(k):
        found = jnp.int32(0)
        for i in range(own):
            found = jnp.where((partner[i, 1] == k) & (screen[i, 1] != 0), 1, found)
        return found

    wanted = [wants(k) for k in range(own)]
    total = sum(wanted)
    lend = (total >= own // 2 + 1) & (total < own)
    ahead, slots = jnp.int32(0), []
    for k in range(own):
        behind = jnp.where(lend, total - 1, total) + k - ahead
        last = jnp.where(lend & (ahead == total - 1), own - 1, ahead)
        slots.append(jnp.where(wanted[k] == 1, last, behind))
        ahead = ahead + wanted[k]
    lane = lax.broadcasted_iota(jnp.int32, (1, 128), 1)
    line = jnp.where(lane == 2 * own, total, 0)
    for k in range(own):
        line = line + jnp.where(lane == k, slots[k], 0)
        turned = sum(jnp.where(slots[j] == k, j, 0) for j in range(own))
        line = line + jnp.where(lane == own + k, turned, 0)
    row[...] = line

    barrier = pltpu.get_barrier_semaphore()

    def place(step):
        other = lax.rem(me + step, groups)
        return (other // n_aux, lax.rem(other, n_aux))

    def greet(step, carry):
        pl.semaphore_signal(barrier, inc=1, device_id=place(step), device_id_type=MESH)
        return carry

    lax.fori_loop(1, groups, greet, 0)
    own_row = pltpu.make_async_copy(row, table.at[me], local)
    own_row.start()
    pl.semaphore_wait(barrier, groups - 1)

    def copy(step, came):
        return pltpu.make_async_remote_copy(
            row, table.at[came], send.at[step], recv.at[step], device_id=place(step), device_id_type=MESH
        )

    def start(step, carry):
        copy(step, me).start()
        return carry

    def finish(step, carry):
        copy(step, lax.rem(me - step + groups, groups)).wait()
        return carry

    lax.fori_loop(1, groups, start, 0)
    own_row.wait()
    lax.fori_loop(1, groups, finish, 0)


def rankings(partner, screen, n_occ, n_aux):
    groups = n_occ * n_aux
    scalars = pl.BlockSpec(memory_space=pltpu.SMEM)
    return pl.pallas_call(
        functools.partial(table_kernel, n_occ, n_aux),
        out_shape=jax.ShapeDtypeStruct((groups, 1, 128), jnp.int32),
        in_specs=[scalars] * 2,
        out_specs=pl.BlockSpec(memory_space=pltpu.VMEM),
        scratch_shapes=[
            pltpu.VMEM((1, 128), jnp.int32),
            pltpu.SemaphoreType.DMA((groups,)),
            pltpu.SemaphoreType.DMA((groups,)),
            pltpu.SemaphoreType.DMA(()),
        ],
        compiler_params=pltpu.CompilerParams(collective_id=0, has_side_effects=True),
    )(partner, screen)


def pack_kernel(base, table, x, out, turned):
    n_aux, own = out.shape[:2]
    turned[...] = pltpu.einshape("qja->jqa", x[...])
    for slot in range(n_aux * own):
        reader = base[0] + slot // own
        out[slot // own, slot % own] = turned[slot // own * own + table[reader, 0, own + slot % own]]


def packed_blocks(x, base, table, n_aux):
    depth, held, nvir = x.shape
    own = held // n_aux
    tile = min(32, depth)
    return pl.pallas_call(
        pack_kernel,
        grid_spec=pltpu.PrefetchScalarGridSpec(
            num_scalar_prefetch=2,
            grid=(depth // tile,),
            in_specs=[pl.BlockSpec((tile, held, nvir), lambda q, *_: (q, 0, 0))],
            out_specs=pl.BlockSpec((n_aux, own, tile, nvir), lambda q, *_: (0, 0, q, 0)),
            scratch_shapes=[pltpu.VMEM((held, tile, nvir), x.dtype)],
        ),
        out_shape=jax.ShapeDtypeStruct((n_aux, own, depth, nvir), x.dtype),
    )(base, table, x)


def peer_of(i, step, n_aux):
    return i ^ step if n_aux & (n_aux - 1) == 0 else lax.rem(step + n_aux - i, n_aux)


def shares(total, own):
    caps = ((total + 1) // 2, total // 2)
    spill = tuple(jnp.minimum(own - caps[1 - c], caps[c]) for c in range(2))
    return caps, spill


def fixed_shares(total, own):
    caps = ((total + 1) // 2, total // 2)
    return caps, tuple(min(own - caps[1 - c], caps[c]) for c in range(2))


def move_kernel(
    total, n_occ, n_aux, ints, floats, packed, mixed, col, row,
    far, begun, coeff, wrapped, fills, amp, block_out,
    pool, lent, stage, term, kept_amp, parts, half, sum1, from_side, from_aux, from_z, gathered,
    sent, came, far_sent, far_came, side_sent, side_came, cross_sent, cross_came,
    wrap_sems, local, stored, fold_sent, fold_came, lend_sent, lend_came,
):
    own, depth = packed.shape[1:3]
    naux, nvir = stage.shape
    occ, aux = lax.axis_index("occ"), lax.axis_index("aux")
    core = lax.rem(occ, 2)
    pick = lambda pair: pair[0] + core * (pair[1] - pair[0])
    caps, spills = fixed_shares(total, own)
    cap, cap_mate, spill, spill_mate = pick(caps), pick(caps[::-1]), pick(spills), pick(spills[::-1])
    pooled = total < 2 * own
    aside = own - min(caps) + 1 if pooled else 0
    most_z = n_occ // 2
    mate = (lax.rem(occ + n_occ // 2, n_occ), aux)
    after = (lax.rem(occ + 1, n_occ), aux)
    before = (lax.rem(occ + n_occ - 1, n_occ), aux)
    side = (occ + 1 - 2 * core, aux)
    above = (occ + 2 - 4 * lax.rem(occ // 2, 2), aux)
    peers = [(occ, peer_of(aux, s, n_aux)) for s in range(n_aux)]
    column = [(lax.rem(occ + 2 * k, n_occ), aux) for k in range(most_z)]
    column_before = [(lax.rem(occ + n_occ - 2 * k, n_occ), aux) for k in range(most_z)]

    barrier = pltpu.get_barrier_semaphore()
    greeted = [after, before, side] + peers[1:] + column[1:]
    for device in greeted:
        pl.semaphore_signal(barrier, inc=1, device_id=device, device_id_type=MESH)
    pl.semaphore_wait(barrier, len(greeted))

    def remote(source, target, send, recv, device):
        return pltpu.make_async_remote_copy(source, target, send, recv, device_id=device, device_id_type=MESH)

    wrap = remote(packed.at[n_aux - 1], wrapped, wrap_sems.at[0], wrap_sems.at[1], after)
    wrap.start()

    def part(land, t, q):
        return land.at[t, pl.ds(pl.multiple_of(q * depth, depth), depth)]

    def piece(kind, land, source, t, s, q):
        if s == 0:
            return pltpu.make_async_copy(source, part(land, t, q), local.at[kind, t])
        return remote(source, part(land, t, q), sent.at[kind, t, s], came.at[kind, t, s], peers[s])

    def send_own(step, carry):
        t = lax.rem(step + own - 1, own) if pooled else step
        for s in range(n_aux):
            piece(0, pool, packed.at[peers[s][1], t], t, s, aux).start()
        return carry

    def send_near(t, carry):
        for s in range(n_aux):
            to = peers[s][1]

            @pl.when(to == 0)
            def _():
                piece(1, lent, wrapped.at[t], t, s, aux).start()

            @pl.when(to != 0)
            def _():
                piece(1, lent, packed.at[jnp.maximum(to - 1, 0), t], t, s, aux).start()

        return carry

    tile = min(256, naux)

    def put(source, target):
        out = pltpu.make_async_copy(source, target, stored)
        out.start()
        out.wait()

    def transform(kind, land, t):
        for s in range(n_aux):
            move = piece(kind, land, packed.at[0, 0], t, s, peers[s][1])
            move.wait() if s == 0 else move.wait_recv()

        def rows(i, carry):
            at = pl.ds(pl.multiple_of(i * tile, tile), tile)
            stage[at, :] = jnp.dot(mixed[at, :], land[t], preferred_element_type=jnp.float32).astype(stage.dtype)
            return carry

        def back(i, carry):
            at = pl.ds(pl.multiple_of(i * tile, tile), tile)
            land[t, at, :] = stage[at, :]
            return carry

        lax.fori_loop(0, naux // tile, rows, 0)
        lax.fori_loop(0, naux // tile, back, 0)

    def far_copy(source, t):
        return remote(source, far.at[t], far_sent.at[t], far_came.at[t], mate)

    def side_copy(t, x):
        return remote(coeff.at[t], pool.at[own + x], side_sent.at[x], side_came.at[x], side)

    def cross_copy(t, f, place):
        return remote(far.at[t], far.at[place + f], cross_sent.at[f], cross_came.at[f], side)

    def lend_copy():
        return remote(coeff.at[own - 1], pool.at[own + aside], lend_sent.at[0], lend_came.at[0], above)

    def back_copy():
        return remote(far.at[cap - spill], far.at[own], lend_sent.at[1], lend_came.at[1], above)

    def own_slot(step, carry):
        t = lax.rem(step + own - 1, own) if pooled else step

        @pl.when(step == min(own - 1, 2))
        def _():
            wrap.wait()
            lax.fori_loop(0, own, send_near, 0)

        transform(0, pool, t)
        put(pool.at[t], coeff.at[t])

        @pl.when(t < cap - spill)
        def _():
            far_copy(coeff.at[t], t).start()

        if pooled:

            @pl.when(t >= cap - 1)
            def _():
                side_copy(t, jnp.maximum(t - (cap - 1), 0)).start()

            @pl.when(t == own - 1)
            def _():
                lend_copy().start()

        return carry

    def relay():
        first = cap - spill
        far_copy(coeff.at[first], first).wait_recv()
        back_copy().start()
        cross_copy(first, 0, cap_mate).start()
        far_copy(fills.at[spill - 1], cap - 1).start()

    def near_slot(t, carry):
        transform(1, lent, t)
        if pooled:

            @pl.when(t == own - 2)
            def _():
                relay()

        return carry

    lax.fori_loop(0, own, send_own, 0)
    lax.fori_loop(0, own, own_slot, 0)

    def side_wait(x, carry):
        side_copy(0, x).wait_recv()
        return carry

    if pooled:
        lax.fori_loop(0, own - cap_mate + 1, side_wait, 0)
        lend_copy().wait_recv()

    def fill(f, carry):
        def copy(i, inner):
            at = pl.ds(pl.multiple_of(i * tile, tile), tile)
            stage[at, :] = pool[ints[2, f], at, :]
            return inner

        lax.fori_loop(0, naux // tile, copy, 0)
        put(stage, fills.at[f])
        @pl.when(f < spill - 1)
        def _():
            far_copy(fills.at[f], cap - spill + f).start()

        return carry

    lax.fori_loop(0, spill, fill, 0)
    lax.fori_loop(0, own, near_slot, 0)

    parts[...] = jnp.zeros_like(parts)

    def amplitude(left, right, kept, gap):
        both = lax.dot_general(left, right, TN, preferred_element_type=jnp.float32)
        block = (kept * both / (col[...] + row[...] - gap[0] - gap[1])).astype(amp.dtype)
        square = lax.dot_general(block, block, NT, preferred_element_type=jnp.float32)
        parts[...] += square.reshape(parts.shape)
        return block

    def pair0(i, carry):
        kept_amp[...] = amplitude(pool[ints[4, i]], lent[ints[0, i]], floats[0, i], (floats[2, i], floats[4, i]))

        def rows(k, inner):
            at = pl.ds(pl.multiple_of(k * tile, tile), tile)
            term[...] = lax.dot_general(
                lent[ints[0, i], at, :], kept_amp[...], NT, preferred_element_type=jnp.float32
            )
            put(term, begun.at[i, at])
            return inner

        lax.fori_loop(0, naux // tile, rows, 0)
        return carry

    lax.fori_loop(0, own, pair0, 0)

    def pair1(m, carry):
        kept_amp[...] = amplitude(pool[ints[5, m]], lent[ints[6, m]], floats[1, m], (floats[3, m], floats[5, m]))
        put(kept_amp, amp.at[m])
        return carry

    def arrive(u, carry):
        @pl.when(u != cap - spill if pooled else u >= 0)
        def _():
            far_copy(coeff.at[u], u).wait_recv()

        if pooled:

            @pl.when(u > cap - spill)
            def _():
                cross_copy(u, jnp.maximum(u - (cap - spill), 0), cap_mate).start()

        put(far.at[u], lent.at[u])
        if pooled:

            @pl.when(u >= 1)
            def _():
                pair1(jnp.maximum(u - 1, 0), 0)

        return carry

    def crossed(f, carry):
        cross_copy(0, f, cap).wait_recv()
        put(far.at[cap + f], lent.at[cap + f])
        return carry

    lax.fori_loop(0, cap, arrive, 0)
    if pooled:
        back_copy().wait_recv()
        put(far.at[own], lent.at[own])
        lax.fori_loop(0, spill_mate, crossed, 0)
    lax.fori_loop(cap - 1 if pooled else 0, own, pair1, 0)

    fold = lambda k, source, target, device: remote(source, target, fold_sent.at[k], fold_came.at[k], device)
    swap = fold(0, parts.at[:, 1 - core], from_side, side)
    swap.start()
    swap.wait()
    half[...] = parts[:, core] + from_side[...]
    moves = [fold(s, half.at[:, peers[s][1]], from_aux.at[s - 1], peers[s]) for s in range(1, n_aux)]
    for move in moves:
        move.start()
    for move in moves:
        move.wait()
    sum1[...] = half[:, aux] + jnp.sum(from_aux[...], axis=0)
    moves = []
    for k in range(1, most_z):
        moves.append(fold(n_aux + k - 1, sum1.at[column[k][0] // 2], from_z.at[k - 1], column[k]))
    for move in moves:
        move.start()
    for move in moves:
        move.wait()
    gathered[aux] = (sum1[occ // 2] + jnp.sum(from_z[...], axis=0)) / NOCC
    base = n_aux + most_z - 2
    moves = [fold(base + s, gathered.at[aux], gathered.at[aux], peers[s]) for s in range(1, n_aux)]
    for move in moves:
        move.start()
    for s, move in enumerate(moves):
        move.wait_send()
        fold(base + s + 1, gathered.at[aux], gathered.at[peers[s + 1][1]], peers[s + 1]).wait_recv()
    block_out[...] = gathered[...].reshape(block_out.shape)

    def drain(t, carry):
        for kind, land in ((0, pool), (1, lent)):
            for s in range(1, n_aux):
                piece(kind, land, packed.at[0, 0], t, s, aux).wait_send()
        return carry

    def side_drain(x, carry):
        side_copy(0, x).wait_send()
        return carry

    def far_drain(t, carry):
        far_copy(coeff.at[t], t).wait_send()
        return carry

    def cross_drain(f, carry):
        cross_copy(0, f, cap_mate).wait_send()
        return carry

    lax.fori_loop(0, own, drain, 0)
    lax.fori_loop(0, cap, far_drain, 0)
    if pooled:
        lax.fori_loop(0, own - cap + 1, side_drain, 0)
        lax.fori_loop(0, spill, cross_drain, 0)
        lend_copy().wait_send()
        back_copy().wait_send()


def moved(packed, mixed, e_vir, ints, floats, total, n_occ, n_aux):
    _, own, depth, nvir = packed.shape
    naux = depth * n_aux
    caps, spills = fixed_shares(total, own)
    spill, aside = max(1, *spills), own - min(caps) + 1 if total < 2 * own else 0
    anywhere = pl.BlockSpec(memory_space=pl.ANY)
    fast = pl.BlockSpec(memory_space=pltpu.VMEM)
    scalars = pl.BlockSpec(memory_space=pltpu.SMEM)
    kind = packed.dtype
    dma = pltpu.SemaphoreType.DMA
    wide = lambda count: jax.ShapeDtypeStruct((count, naux, nvir), kind)
    most_z, thin = n_occ // 2, nvir // (n_occ * n_aux)
    single = lambda *lead: pltpu.VMEM(lead + (thin, nvir), jnp.float32)
    folds = 2 * n_aux + most_z - 1
    return pl.pallas_call(
        functools.partial(move_kernel, total, n_occ, n_aux),
        out_shape=[
            wide(own + 1),
            jax.ShapeDtypeStruct((own, naux, nvir), jnp.float32),
            wide(own),
            jax.ShapeDtypeStruct((own, depth, nvir), kind),
            wide(spill),
            jax.ShapeDtypeStruct((own, nvir, nvir), kind),
            jax.ShapeDtypeStruct((nvir // n_occ, nvir), jnp.float32),
        ],
        in_specs=[scalars] * 2 + [anywhere, fast, fast, fast],
        out_specs=[anywhere] * 6 + [fast],
        scratch_shapes=[
            pltpu.VMEM((own + aside + 1, naux, nvir), kind),
            pltpu.VMEM((own + 1, naux, nvir), kind),
            pltpu.VMEM((naux, nvir), kind),
            pltpu.VMEM((min(256, naux), nvir), jnp.float32),
            pltpu.VMEM((nvir, nvir), kind),
            single(most_z, 2, n_aux),
            single(most_z, n_aux),
            single(most_z),
            single(most_z, n_aux),
            single(n_aux - 1, most_z),
            single(most_z - 1),
            single(n_aux),
            dma((2, own, n_aux)),
            dma((2, own, n_aux)),
            dma((own,)),
            dma((own,)),
            dma((max(1, aside),)),
            dma((max(1, aside),)),
            dma((spill,)),
            dma((spill,)),
            dma((2,)),
            dma((2, own)),
            dma(()),
            dma((folds,)),
            dma((folds,)),
            dma((2,)),
            dma((2,)),
        ],
        compiler_params=pltpu.CompilerParams(
            collective_id=total, has_side_effects=True, vmem_limit_bytes=67043328
        ),
    )(ints, floats, packed, mixed, e_vir[:, None], e_vir[None, :])


def lending(total, own, wanted):
    caps, spill = shares(total, own)
    over = [wanted[z][0] + wanted[z][1] - total for z in range(2)]
    flag = lambda test: jnp.where(test, 1, 0)
    lends = []
    for z in range(2):
        big = [wanted[z][c] > caps[c] for c in range(2)]
        one, two = over[z] == 1, over[z] == 2
        lends.append([flag((one & big[0]) | two), flag((one & jnp.logical_not(big[0])) | two)])
    fine, items, excess = True, [], []
    for z in range(2):
        fine = fine & (over[z] <= 2)
        for c in range(2):
            fine = fine & ((lends[z][c] == 0) | (wanted[z][c] > caps[c]))
        items.append(
            [lends[1 - z][c] + jnp.maximum(wanted[z][c] - caps[c] + spill[c], 0) - lends[z][c] for c in range(2)]
        )
        excess.append([jnp.maximum(items[z][c] - spill[c], 0) for c in range(2)])
        for c in range(2):
            fine = fine & (jnp.minimum(items[z][c], spill[c]) + excess[z][1 - c] <= spill[c])
            fine = fine & ((lends[z][0] + lends[z][1] == 0) | (lends[1 - z][c] == 0))
    return lends, items, excess, fine


def plan_kernel(choices, n_occ, n_aux, table, partner, screen, e_occ, ints, floats, branch):
    groups = n_occ * n_aux
    own = partner.shape[0]
    occ, aux = lax.axis_index("occ"), lax.axis_index("aux")
    device = occ * n_aux + aux
    far_by = groups // 2
    reader = lambda source: lax.rem(source + far_by, groups)
    slot_of = lambda source, orbital: table[reader(source), 0, orbital]

    def counts(first):
        count = lambda o: table[reader(o * n_aux + aux_of), 0, 2 * own]
        aux_of = lax.rem(first, n_aux)
        row = first // n_aux
        return [[count(row + 2 * z + c) for c in range(2)] for z in range(2)]

    chosen, total = jnp.int32(0), jnp.int32(choices[0])
    for k in range(1, len(choices)):

        def quad(q, good):
            first = q // n_aux * 4 * n_aux + lax.rem(q, n_aux)
            return good & jnp.where(lending(choices[k - 1], own, counts(first))[3], 1, 0)

        over = lax.fori_loop(0, groups // 4, quad, jnp.int32(1)) == 0
        still = over & (chosen == k - 1)
        chosen = jnp.where(still, k, chosen)
        total = jnp.where(still, choices[k], total)
    branch[0] = chosen
    pooled = total < 2 * own
    caps, spills = shares(total, own)
    core = lax.rem(occ, 2)
    level = lax.rem(occ // 2, 2)
    by_core = lambda pair, c: jnp.where(c == 0, pair[0], pair[1])
    at = lambda grid, z, c: by_core([by_core(grid[0], c), by_core(grid[1], c)], z)
    cap, cap_mate = by_core(caps, core), by_core(caps, 1 - core)
    spill, spill_mate = by_core(spills, core), by_core(spills, 1 - core)
    aside = own - caps[1] + 1
    many = own // 2 + 1

    def shared_slot(item, first_shared, wanted):
        lent = (wanted >= many) & (item == wanted - 1 - first_shared)
        return jnp.where(lent, own - 1, first_shared + item)

    wanted = counts((occ - 2 * level - core) * n_aux + aux)
    lends, items, excess, _ = lending(total, own, wanted)
    carries, mine, theirs = at(lends, 1 - level, core), at(items, level, core), at(excess, level, 1 - core)
    wanted_own, wanted_side = at(wanted, level, core), at(wanted, level, 1 - core)
    side_carries = at(lends, 1 - level, 1 - core)
    for f in range(own):
        own_item = shared_slot(f - carries, cap - spill, wanted_own)
        k = f - mine
        side_slot = shared_slot(spill_mate - side_carries + k, cap_mate - spill_mate, wanted_side)
        side_item = jnp.where(k < theirs, own + side_slot - (cap_mate - 1), 0)
        item = jnp.where(f < mine, own_item, side_item)
        item = jnp.where((f == 0) & (carries == 1), own + aside, item)
        ints[2, f] = jnp.where(pooled, jnp.clip(item, 0, own + aside), 0)

    near, far = lax.rem(device + groups - 1, groups), lax.rem(device + groups - far_by, groups)
    source_occ = far // n_aux
    wanted = counts((source_occ - 2 * level - core) * n_aux + aux)
    lends, items, _, _ = lending(total, own, wanted)
    lent_one, carries = at(lends, level, core), at(lends, 1 - level, core)
    wanted_own = at(wanted, level, core)
    side_items = jnp.minimum(at(items, level, 1 - core), spill_mate)

    def far_slot(slot):
        special = (slot == own - 1) & (wanted_own >= many)
        item = jnp.where(special, wanted_own - 1 - (cap - spill), slot - (cap - spill))
        f = carries + item
        shared = jnp.where(f < spill, cap - spill + f, cap + side_items + f - spill)
        place = jnp.where(special & (lent_one == 1), own, shared)
        place = jnp.where(slot < cap - spill, slot, place)
        return jnp.clip(place, 0, own)

    found = [far_slot(slot_of(far, partner[i, 1])) for i in range(own)]
    found = [jnp.where(screen[i, 1] != 0, found[i], 0) for i in range(own)]
    keys = [jnp.where(screen[i, 1] != 0, found[i], own + 1) for i in range(own)]
    for i in range(own):
        ints[0, i] = slot_of(near, partner[i, 0])
        ints[1, i] = found[i]
        where = jnp.int32(0)
        for other in range(own):
            if other != i:
                ahead = keys[other] < keys[i] if other > i else keys[other] <= keys[i]
                where = where + jnp.where(ahead, 1, 0)
        ints[3, i] = where
        mine = slot_of(device, i)
        ints[4, i] = mine
        ints[5, where] = mine
        ints[6, where] = found[i]
        floats[0, i] = screen[i, 0].astype(jnp.float32)
        floats[1, where] = screen[i, 1].astype(jnp.float32)
        energy = e_occ[device * own + i]
        floats[2, i] = energy
        floats[3, where] = energy
        floats[4, i] = e_occ[near * own + partner[i, 0]]
        floats[5, where] = e_occ[far * own + partner[i, 1]]


def plan(choices, table, partner, screen, e_occ, n_occ, n_aux):
    own = partner.shape[0]
    scalars = pl.BlockSpec(memory_space=pltpu.SMEM)
    return pl.pallas_call(
        functools.partial(plan_kernel, choices, n_occ, n_aux),
        out_shape=[
            jax.ShapeDtypeStruct((7, own), jnp.int32),
            jax.ShapeDtypeStruct((6, own), jnp.float32),
            jax.ShapeDtypeStruct((1,), jnp.int32),
        ],
        in_specs=[scalars] * 4,
        out_specs=[scalars] * 3,
    )(table, partner, screen, e_occ)


def on_device(integrals, metric, e_occ, e_vir, partner, screen):
    n_occ, n_aux = lax.axis_size("occ"), lax.axis_size("aux")
    groups = n_occ * n_aux
    depth, held, nvir = integrals.shape
    own = held // n_aux
    occ, aux = lax.axis_index("occ"), lax.axis_index("aux")
    device = occ * n_aux + aux

    table = rankings(partner, screen, n_occ, n_aux)

    reader = ((occ + n_occ // 2) % n_occ) * n_aux
    packed = packed_blocks(integrals, reader[None], table, n_aux)

    choices = sorted(set(range(own + 1, 2 * own - 3)) | {2 * own})
    ints, floats, branch = plan(choices, table, partner, screen, e_occ, n_occ, n_aux)

    def chosen(total):
        far, begun, _, _, _, amp, block = moved(packed, metric, e_vir, ints, floats, total, n_occ, n_aux)
        return far, begun, amp, block

    far, begun, amp, block = lax.switch(branch[0], [functools.partial(chosen, total) for total in choices])
    return gradient(far, amp, begun, ints), block


def solution(mesh):
    return jax.shard_map(
        on_device,
        mesh=mesh,
        in_specs=(P("aux", "occ", None), P(), P(), P(), P(BOTH, None), P(BOTH, None)),
        out_specs=(P(None, BOTH, None), P("occ", None)),
        check_vma=False,
    )
```

```python
import functools

import jax
import jax.numpy as jnp
from jax import lax
from jax.experimental import pallas as pl
from jax.experimental.pallas import tpu as pltpu
from jax.sharding import PartitionSpec as P

NOCC = 256
ROUNDS = 2
BOTH = ("occ", "aux")
NT = (((1,), (1,)), ((), ()))
TN = (((0,), (0,)), ((), ()))

MESH = pl.DeviceIdType.MESH


def gamma_kernel(own, at, right, amp, begun, out, rows):
    now = lax.rem(pl.program_id(0), 2)
    for i in range(own):
        term = lax.dot_general(right[at[1, i]], amp[at[3, i]], NT, preferred_element_type=jnp.float32)
        rows[now, i] = (begun[i] + term).astype(rows.dtype)
    out[...] = pltpu.einshape("ipa->pia", rows[1 - now])


def gradient(right, amp, begun, ints):
    slots, naux, nvir = right.shape
    own = amp.shape[0]
    tile = min(256, naux)
    tiles = naux // tile
    this = lambda p, *_: (0, jnp.minimum(p, tiles - 1), 0)
    return pl.pallas_call(
        functools.partial(gamma_kernel, own),
        grid_spec=pltpu.PrefetchScalarGridSpec(
            num_scalar_prefetch=1,
            grid=(tiles + 1,),
            in_specs=[
                pl.BlockSpec((slots, tile, nvir), this),
                pl.BlockSpec(amp.shape, lambda p, *_: (0, 0, 0)),
                pl.BlockSpec((own, tile, nvir), this),
            ],
            out_specs=pl.BlockSpec((tile, own, nvir), lambda p, *_: (jnp.maximum(p - 1, 0), 0, 0)),
            scratch_shapes=[pltpu.VMEM((2, own, tile, nvir), jnp.bfloat16)],
        ),
        out_shape=jax.ShapeDtypeStruct((naux, own, nvir), jnp.bfloat16),
    )(ints, right, amp, begun)


def table_kernel(n_occ, n_aux, partner, screen, table, row, send, recv, local):
    groups = n_occ * n_aux
    own = partner.shape[0]
    me = lax.axis_index("occ") * n_aux + lax.axis_index("aux")

    def wants(k):
        found = jnp.int32(0)
        for i in range(own):
            found = jnp.where((partner[i, 1] == k) & (screen[i, 1] != 0), 1, found)
        return found

    wanted = [wants(k) for k in range(own)]
    total = sum(wanted)
    lend = (total >= own // 2 + 1) & (total < own)
    ahead, slots = jnp.int32(0), []
    for k in range(own):
        behind = jnp.where(lend, total - 1, total) + k - ahead
        last = jnp.where(lend & (ahead == total - 1), own - 1, ahead)
        slots.append(jnp.where(wanted[k] == 1, last, behind))
        ahead = ahead + wanted[k]
    lane = lax.broadcasted_iota(jnp.int32, (1, 128), 1)
    line = jnp.where(lane == 2 * own, total, 0)
    for k in range(own):
        line = line + jnp.where(lane == k, slots[k], 0)
        turned = sum(jnp.where(slots[j] == k, j, 0) for j in range(own))
        line = line + jnp.where(lane == own + k, turned, 0)
    row[...] = line

    barrier = pltpu.get_barrier_semaphore()

    def place(step):
        other = lax.rem(me + step, groups)
        return (other // n_aux, lax.rem(other, n_aux))

    def greet(step, carry):
        pl.semaphore_signal(barrier, inc=1, device_id=place(step), device_id_type=MESH)
        return carry

    lax.fori_loop(1, groups, greet, 0)
    own_row = pltpu.make_async_copy(row, table.at[me], local)
    own_row.start()
    pl.semaphore_wait(barrier, groups - 1)

    def copy(step, came):
        return pltpu.make_async_remote_copy(
            row, table.at[came], send.at[step], recv.at[step], device_id=place(step), device_id_type=MESH
        )

    def start(step, carry):
        copy(step, me).start()
        return carry

    def finish(step, carry):
        copy(step, lax.rem(me - step + groups, groups)).wait()
        return carry

    lax.fori_loop(1, groups, start, 0)
    own_row.wait()
    lax.fori_loop(1, groups, finish, 0)


def rankings(partner, screen, n_occ, n_aux):
    groups = n_occ * n_aux
    scalars = pl.BlockSpec(memory_space=pltpu.SMEM)
    return pl.pallas_call(
        functools.partial(table_kernel, n_occ, n_aux),
        out_shape=jax.ShapeDtypeStruct((groups, 1, 128), jnp.int32),
        in_specs=[scalars] * 2,
        out_specs=pl.BlockSpec(memory_space=pltpu.VMEM),
        scratch_shapes=[
            pltpu.VMEM((1, 128), jnp.int32),
            pltpu.SemaphoreType.DMA((groups,)),
            pltpu.SemaphoreType.DMA((groups,)),
            pltpu.SemaphoreType.DMA(()),
        ],
        compiler_params=pltpu.CompilerParams(collective_id=0, has_side_effects=True),
    )(partner, screen)


def pack_kernel(base, table, x, out, turned):
    n_aux, own = out.shape[:2]
    turned[...] = pltpu.einshape("qja->jqa", x[...])
    for slot in range(n_aux * own):
        reader = base[0] + slot // own
        out[slot // own, slot % own] = turned[slot // own * own + table[reader, 0, own + slot % own]]


def packed_blocks(x, base, table, n_aux):
    depth, held, nvir = x.shape
    own = held // n_aux
    tile = min(32, depth)
    return pl.pallas_call(
        pack_kernel,
        grid_spec=pltpu.PrefetchScalarGridSpec(
            num_scalar_prefetch=2,
            grid=(depth // tile,),
            in_specs=[pl.BlockSpec((tile, held, nvir), lambda q, *_: (q, 0, 0))],
            out_specs=pl.BlockSpec((n_aux, own, tile, nvir), lambda q, *_: (0, 0, q, 0)),
            scratch_shapes=[pltpu.VMEM((held, tile, nvir), x.dtype)],
        ),
        out_shape=jax.ShapeDtypeStruct((n_aux, own, depth, nvir), x.dtype),
    )(base, table, x)


def peer_of(i, step, n_aux):
    return i ^ step if n_aux & (n_aux - 1) == 0 else lax.rem(step + n_aux - i, n_aux)


def shares(total, own):
    caps = ((total + 1) // 2, total // 2)
    spill = tuple(jnp.minimum(own - caps[1 - c], jnp.maximum(caps[c] - 2, 0)) for c in range(2))
    return caps, spill


def fixed_shares(total, own):
    caps = ((total + 1) // 2, total // 2)
    return caps, tuple(min(own - caps[1 - c], max(caps[c] - 2, 0)) for c in range(2))


def move_kernel(
    total, n_occ, n_aux, ints, floats, packed, mixed, col, row,
    far, begun, coeff, wrapped, fills, amp, block_out,
    pool, lent, stage, term, kept_amp, parts, half, sum1, from_side, from_aux, from_z, gathered,
    sent, came, far_sent, far_came, side_sent, side_came, cross_sent, cross_came,
    wrap_sems, local, stored, fold_sent, fold_came, lend_sent, lend_came,
):
    own, depth = packed.shape[1:3]
    naux, nvir = stage.shape
    occ, aux = lax.axis_index("occ"), lax.axis_index("aux")
    core = lax.rem(occ, 2)
    pick = lambda pair: pair[0] + core * (pair[1] - pair[0])
    caps, spills = fixed_shares(total, own)
    cap, cap_mate, spill, spill_mate = pick(caps), pick(caps[::-1]), pick(spills), pick(spills[::-1])
    pooled = total < 2 * own
    aside = own - min(caps) + 1 if pooled else 0
    most_z = n_occ // 2
    mate = (lax.rem(occ + n_occ // 2, n_occ), aux)
    after = (lax.rem(occ + 1, n_occ), aux)
    before = (lax.rem(occ + n_occ - 1, n_occ), aux)
    side = (occ + 1 - 2 * core, aux)
    above = (occ + 2 - 4 * lax.rem(occ // 2, 2), aux)
    peers = [(occ, peer_of(aux, s, n_aux)) for s in range(n_aux)]
    column = [(lax.rem(occ + 2 * k, n_occ), aux) for k in range(most_z)]
    column_before = [(lax.rem(occ + n_occ - 2 * k, n_occ), aux) for k in range(most_z)]

    barrier = pltpu.get_barrier_semaphore()
    greeted = [after, before, side] + peers[1:] + column[1:]
    for device in greeted:
        pl.semaphore_signal(barrier, inc=1, device_id=device, device_id_type=MESH)
    pl.semaphore_wait(barrier, len(greeted))

    def remote(source, target, send, recv, device):
        return pltpu.make_async_remote_copy(source, target, send, recv, device_id=device, device_id_type=MESH)

    wrap = remote(packed.at[n_aux - 1], wrapped, wrap_sems.at[0], wrap_sems.at[1], after)
    wrap.start()

    def part(land, t, q):
        return land.at[t, pl.ds(pl.multiple_of(q * depth, depth), depth)]

    def piece(kind, land, source, t, s, q):
        if s == 0:
            return pltpu.make_async_copy(source, part(land, t, q), local.at[kind, t])
        return remote(source, part(land, t, q), sent.at[kind, t, s], came.at[kind, t, s], peers[s])

    def send_own(step, carry):
        t = lax.rem(step + own - 1, own) if pooled else step
        for s in range(n_aux):
            piece(0, pool, packed.at[peers[s][1], t], t, s, aux).start()
        return carry

    def send_near(t, carry):
        for s in range(n_aux):
            to = peers[s][1]

            @pl.when(to == 0)
            def _():
                piece(1, lent, wrapped.at[t], t, s, aux).start()

            @pl.when(to != 0)
            def _():
                piece(1, lent, packed.at[jnp.maximum(to - 1, 0), t], t, s, aux).start()

        return carry

    tile = min(256, naux)

    def put(source, target):
        out = pltpu.make_async_copy(source, target, stored)
        out.start()
        out.wait()

    def transform(kind, land, t):
        for s in range(n_aux):
            move = piece(kind, land, packed.at[0, 0], t, s, peers[s][1])
            move.wait() if s == 0 else move.wait_recv()

        def rows(i, carry):
            at = pl.ds(pl.multiple_of(i * tile, tile), tile)
            stage[at, :] = jnp.dot(mixed[at, :], land[t], preferred_element_type=jnp.float32).astype(stage.dtype)
            return carry

        def back(i, carry):
            at = pl.ds(pl.multiple_of(i * tile, tile), tile)
            land[t, at, :] = stage[at, :]
            return carry

        lax.fori_loop(0, naux // tile, rows, 0)
        lax.fori_loop(0, naux // tile, back, 0)

    def far_copy(source, t):
        return remote(source, far.at[t], far_sent.at[t], far_came.at[t], mate)

    def side_copy(t, x):
        return remote(coeff.at[t], pool.at[own + x], side_sent.at[x], side_came.at[x], side)

    def cross_copy(t, f, place):
        return remote(far.at[t], far.at[place + f], cross_sent.at[f], cross_came.at[f], side)

    def lend_copy():
        return remote(coeff.at[own - 1], pool.at[own + aside], lend_sent.at[0], lend_came.at[0], above)

    def back_copy():
        return remote(far.at[cap - spill], far.at[own], lend_sent.at[1], lend_came.at[1], above)

    def own_slot(step, carry):
        t = lax.rem(step + own - 1, own) if pooled else step

        @pl.when(step == min(own - 1, 2))
        def _():
            wrap.wait()
            lax.fori_loop(0, own, send_near, 0)

        transform(0, pool, t)
        put(pool.at[t], coeff.at[t])

        @pl.when(t < cap - spill)
        def _():
            far_copy(coeff.at[t], t).start()

        if pooled:

            @pl.when(t >= cap - 1)
            def _():
                side_copy(t, jnp.maximum(t - (cap - 1), 0)).start()

            @pl.when(t == own - 1)
            def _():
                lend_copy().start()

        return carry

    def relay():
        first = cap - spill
        far_copy(coeff.at[first], first).wait_recv()
        back_copy().start()
        cross_copy(first, 0, cap_mate).start()
        far_copy(fills.at[spill - 1], cap - 1).start()

    def near_slot(t, carry):
        transform(1, lent, t)
        if pooled:

            @pl.when(t == own - 2)
            def _():
                relay()

        return carry

    lax.fori_loop(0, own, send_own, 0)
    lax.fori_loop(0, own, own_slot, 0)

    def side_wait(x, carry):
        side_copy(0, x).wait_recv()
        return carry

    if pooled:
        lax.fori_loop(0, own - cap_mate + 1, side_wait, 0)
        lend_copy().wait_recv()

    def fill(f, carry):
        def copy(i, inner):
            at = pl.ds(pl.multiple_of(i * tile, tile), tile)
            stage[at, :] = pool[ints[2, f], at, :]
            return inner

        lax.fori_loop(0, naux // tile, copy, 0)
        put(stage, fills.at[f])
        @pl.when(f < spill - 1)
        def _():
            far_copy(fills.at[f], cap - spill + f).start()

        return carry

    lax.fori_loop(0, spill, fill, 0)
    lax.fori_loop(0, own, near_slot, 0)

    parts[...] = jnp.zeros_like(parts)

    def amplitude(left, right, kept, gap):
        both = lax.dot_general(left, right, TN, preferred_element_type=jnp.float32)
        block = (kept * both / (col[...] + row[...] - gap[0] - gap[1])).astype(amp.dtype)
        square = lax.dot_general(block, block, NT, preferred_element_type=jnp.float32)
        parts[...] += square.reshape(parts.shape)
        return block

    def pair0(i, carry):
        kept_amp[...] = amplitude(pool[ints[4, i]], lent[ints[0, i]], floats[0, i], (floats[2, i], floats[4, i]))

        def rows(k, inner):
            at = pl.ds(pl.multiple_of(k * tile, tile), tile)
            term[...] = lax.dot_general(
                lent[ints[0, i], at, :], kept_amp[...], NT, preferred_element_type=jnp.float32
            )
            put(term, begun.at[i, at])
            return inner

        lax.fori_loop(0, naux // tile, rows, 0)
        return carry

    lax.fori_loop(0, own, pair0, 0)

    def pair1(m, carry):
        kept_amp[...] = amplitude(pool[ints[5, m]], lent[ints[6, m]], floats[1, m], (floats[3, m], floats[5, m]))
        put(kept_amp, amp.at[m])
        return carry

    def arrive(u, carry):
        @pl.when(u != cap - spill if pooled else u >= 0)
        def _():
            far_copy(coeff.at[u], u).wait_recv()

        if pooled:

            @pl.when(u > cap - spill)
            def _():
                cross_copy(u, jnp.maximum(u - (cap - spill), 0), cap_mate).start()

        put(far.at[u], lent.at[u])
        if pooled:

            @pl.when(u >= 1)
            def _():
                pair1(jnp.maximum(u - 1, 0), 0)

        return carry

    def crossed(f, carry):
        cross_copy(0, f, cap).wait_recv()
        put(far.at[cap + f], lent.at[cap + f])
        return carry

    lax.fori_loop(0, cap, arrive, 0)
    if pooled:
        back_copy().wait_recv()
        put(far.at[own], lent.at[own])
        lax.fori_loop(0, spill_mate, crossed, 0)
    lax.fori_loop(cap - 1 if pooled else 0, own, pair1, 0)

    fold = lambda k, source, target, device: remote(source, target, fold_sent.at[k], fold_came.at[k], device)
    swap = fold(0, parts.at[:, 1 - core], from_side, side)
    swap.start()
    swap.wait()
    half[...] = parts[:, core] + from_side[...]
    moves = [fold(s, half.at[:, peers[s][1]], from_aux.at[s - 1], peers[s]) for s in range(1, n_aux)]
    for move in moves:
        move.start()
    for move in moves:
        move.wait()
    sum1[...] = half[:, aux] + jnp.sum(from_aux[...], axis=0)
    moves = []
    for k in range(1, most_z):
        moves.append(fold(n_aux + k - 1, sum1.at[column[k][0] // 2], from_z.at[k - 1], column[k]))
    for move in moves:
        move.start()
    for move in moves:
        move.wait()
    gathered[aux] = (sum1[occ // 2] + jnp.sum(from_z[...], axis=0)) / NOCC
    base = n_aux + most_z - 2
    moves = [fold(base + s, gathered.at[aux], gathered.at[aux], peers[s]) for s in range(1, n_aux)]
    for move in moves:
        move.start()
    for s, move in enumerate(moves):
        move.wait_send()
        fold(base + s + 1, gathered.at[aux], gathered.at[peers[s + 1][1]], peers[s + 1]).wait_recv()
    block_out[...] = gathered[...].reshape(block_out.shape)

    def drain(t, carry):
        for kind, land in ((0, pool), (1, lent)):
            for s in range(1, n_aux):
                piece(kind, land, packed.at[0, 0], t, s, aux).wait_send()
        return carry

    def side_drain(x, carry):
        side_copy(0, x).wait_send()
        return carry

    def far_drain(t, carry):
        far_copy(coeff.at[t], t).wait_send()
        return carry

    def cross_drain(f, carry):
        cross_copy(0, f, cap_mate).wait_send()
        return carry

    lax.fori_loop(0, own, drain, 0)
    lax.fori_loop(0, cap, far_drain, 0)
    if pooled:
        lax.fori_loop(0, own - cap + 1, side_drain, 0)
        lax.fori_loop(0, spill, cross_drain, 0)
        lend_copy().wait_send()
        back_copy().wait_send()


def moved(packed, mixed, e_vir, ints, floats, total, n_occ, n_aux):
    _, own, depth, nvir = packed.shape
    naux = depth * n_aux
    caps, spills = fixed_shares(total, own)
    spill, aside = max(1, *spills), own - min(caps) + 1 if total < 2 * own else 0
    anywhere = pl.BlockSpec(memory_space=pl.ANY)
    fast = pl.BlockSpec(memory_space=pltpu.VMEM)
    scalars = pl.BlockSpec(memory_space=pltpu.SMEM)
    kind = packed.dtype
    dma = pltpu.SemaphoreType.DMA
    wide = lambda count: jax.ShapeDtypeStruct((count, naux, nvir), kind)
    most_z, thin = n_occ // 2, nvir // (n_occ * n_aux)
    single = lambda *lead: pltpu.VMEM(lead + (thin, nvir), jnp.float32)
    folds = 2 * n_aux + most_z - 1
    return pl.pallas_call(
        functools.partial(move_kernel, total, n_occ, n_aux),
        out_shape=[
            wide(own + 1),
            jax.ShapeDtypeStruct((own, naux, nvir), jnp.float32),
            wide(own),
            jax.ShapeDtypeStruct((own, depth, nvir), kind),
            wide(spill),
            jax.ShapeDtypeStruct((own, nvir, nvir), kind),
            jax.ShapeDtypeStruct((nvir // n_occ, nvir), jnp.float32),
        ],
        in_specs=[scalars] * 2 + [anywhere, fast, fast, fast],
        out_specs=[anywhere] * 6 + [fast],
        scratch_shapes=[
            pltpu.VMEM((own + aside + 1, naux, nvir), kind),
            pltpu.VMEM((own + 1, naux, nvir), kind),
            pltpu.VMEM((naux, nvir), kind),
            pltpu.VMEM((min(256, naux), nvir), jnp.float32),
            pltpu.VMEM((nvir, nvir), kind),
            single(most_z, 2, n_aux),
            single(most_z, n_aux),
            single(most_z),
            single(most_z, n_aux),
            single(n_aux - 1, most_z),
            single(most_z - 1),
            single(n_aux),
            dma((2, own, n_aux)),
            dma((2, own, n_aux)),
            dma((own,)),
            dma((own,)),
            dma((max(1, aside),)),
            dma((max(1, aside),)),
            dma((spill,)),
            dma((spill,)),
            dma((2,)),
            dma((2, own)),
            dma(()),
            dma((folds,)),
            dma((folds,)),
            dma((2,)),
            dma((2,)),
        ],
        compiler_params=pltpu.CompilerParams(
            collective_id=total, has_side_effects=True, vmem_limit_bytes=67043328
        ),
    )(ints, floats, packed, mixed, e_vir[:, None], e_vir[None, :])


def lending(total, own, wanted):
    caps, spill = shares(total, own)
    over = [wanted[z][0] + wanted[z][1] - total for z in range(2)]
    flag = lambda test: jnp.where(test, 1, 0)
    lends = []
    for z in range(2):
        big = [wanted[z][c] > caps[c] for c in range(2)]
        one, two = over[z] == 1, over[z] == 2
        lends.append([flag((one & big[0]) | two), flag((one & jnp.logical_not(big[0])) | two)])
    fine, items, excess = True, [], []
    for z in range(2):
        fine = fine & (over[z] <= 2)
        for c in range(2):
            fine = fine & ((lends[z][c] == 0) | (wanted[z][c] > caps[c]))
        items.append(
            [lends[1 - z][c] + jnp.maximum(wanted[z][c] - caps[c] + spill[c], 0) - lends[z][c] for c in range(2)]
        )
        excess.append([jnp.maximum(items[z][c] - spill[c], 0) for c in range(2)])
        for c in range(2):
            fine = fine & (jnp.minimum(items[z][c], spill[c]) + excess[z][1 - c] <= spill[c])
            fine = fine & ((lends[z][0] + lends[z][1] == 0) | (lends[1 - z][c] == 0))
    return lends, items, excess, fine


def plan_kernel(choices, n_occ, n_aux, table, partner, screen, e_occ, ints, floats, branch):
    groups = n_occ * n_aux
    own = partner.shape[0]
    occ, aux = lax.axis_index("occ"), lax.axis_index("aux")
    device = occ * n_aux + aux
    far_by = groups // 2
    reader = lambda source: lax.rem(source + far_by, groups)
    slot_of = lambda source, orbital: table[reader(source), 0, orbital]

    def counts(first):
        count = lambda o: table[reader(o * n_aux + aux_of), 0, 2 * own]
        aux_of = lax.rem(first, n_aux)
        row = first // n_aux
        return [[count(row + 2 * z + c) for c in range(2)] for z in range(2)]

    chosen, total = jnp.int32(0), jnp.int32(choices[0])
    for k in range(1, len(choices)):

        def quad(q, good):
            first = q // n_aux * 4 * n_aux + lax.rem(q, n_aux)
            return good & jnp.where(lending(choices[k - 1], own, counts(first))[3], 1, 0)

        over = lax.fori_loop(0, groups // 4, quad, jnp.int32(1)) == 0
        still = over & (chosen == k - 1)
        chosen = jnp.where(still, k, chosen)
        total = jnp.where(still, choices[k], total)
    branch[0] = chosen
    pooled = total < 2 * own
    caps, spills = shares(total, own)
    core = lax.rem(occ, 2)
    level = lax.rem(occ // 2, 2)
    by_core = lambda pair, c: jnp.where(c == 0, pair[0], pair[1])
    at = lambda grid, z, c: by_core([by_core(grid[0], c), by_core(grid[1], c)], z)
    cap, cap_mate = by_core(caps, core), by_core(caps, 1 - core)
    spill, spill_mate = by_core(spills, core), by_core(spills, 1 - core)
    aside = own - caps[1] + 1
    many = own // 2 + 1

    def shared_slot(item, first_shared, wanted):
        lent = (wanted >= many) & (item == wanted - 1 - first_shared)
        return jnp.where(lent, own - 1, first_shared + item)

    wanted = counts((occ - 2 * level - core) * n_aux + aux)
    lends, items, excess, _ = lending(total, own, wanted)
    carries, mine, theirs = at(lends, 1 - level, core), at(items, level, core), at(excess, level, 1 - core)
    wanted_own, wanted_side = at(wanted, level, core), at(wanted, level, 1 - core)
    side_carries = at(lends, 1 - level, 1 - core)
    for f in range(own):
        own_item = shared_slot(f - carries, cap - spill, wanted_own)
        k = f - mine
        side_slot = shared_slot(spill_mate - side_carries + k, cap_mate - spill_mate, wanted_side)
        side_item = jnp.where(k < theirs, own + side_slot - (cap_mate - 1), 0)
        item = jnp.where(f < mine, own_item, side_item)
        item = jnp.where((f == 0) & (carries == 1), own + aside, item)
        ints[2, f] = jnp.where(pooled, jnp.clip(item, 0, own + aside), 0)

    near, far = lax.rem(device + groups - 1, groups), lax.rem(device + groups - far_by, groups)
    source_occ = far // n_aux
    wanted = counts((source_occ - 2 * level - core) * n_aux + aux)
    lends, items, _, _ = lending(total, own, wanted)
    lent_one, carries = at(lends, level, core), at(lends, 1 - level, core)
    wanted_own = at(wanted, level, core)
    side_items = jnp.minimum(at(items, level, 1 - core), spill_mate)

    def far_slot(slot):
        special = (slot == own - 1) & (wanted_own >= many)
        item = jnp.where(special, wanted_own - 1 - (cap - spill), slot - (cap - spill))
        f = carries + item
        shared = jnp.where(f < spill, cap - spill + f, cap + side_items + f - spill)
        place = jnp.where(special & (lent_one == 1), own, shared)
        place = jnp.where(slot < cap - spill, slot, place)
        return jnp.clip(place, 0, own)

    found = [far_slot(slot_of(far, partner[i, 1])) for i in range(own)]
    found = [jnp.where(screen[i, 1] != 0, found[i], 0) for i in range(own)]
    keys = [jnp.where(screen[i, 1] != 0, found[i], own + 1) for i in range(own)]
    for i in range(own):
        ints[0, i] = slot_of(near, partner[i, 0])
        ints[1, i] = found[i]
        where = jnp.int32(0)
        for other in range(own):
            if other != i:
                ahead = keys[other] < keys[i] if other > i else keys[other] <= keys[i]
                where = where + jnp.where(ahead, 1, 0)
        ints[3, i] = where
        mine = slot_of(device, i)
        ints[4, i] = mine
        ints[5, where] = mine
        ints[6, where] = found[i]
        floats[0, i] = screen[i, 0].astype(jnp.float32)
        floats[1, where] = screen[i, 1].astype(jnp.float32)
        energy = e_occ[device * own + i]
        floats[2, i] = energy
        floats[3, where] = energy
        floats[4, i] = e_occ[near * own + partner[i, 0]]
        floats[5, where] = e_occ[far * own + partner[i, 1]]


def plan(choices, table, partner, screen, e_occ, n_occ, n_aux):
    own = partner.shape[0]
    scalars = pl.BlockSpec(memory_space=pltpu.SMEM)
    return pl.pallas_call(
        functools.partial(plan_kernel, choices, n_occ, n_aux),
        out_shape=[
            jax.ShapeDtypeStruct((7, own), jnp.int32),
            jax.ShapeDtypeStruct((6, own), jnp.float32),
            jax.ShapeDtypeStruct((1,), jnp.int32),
        ],
        in_specs=[scalars] * 4,
        out_specs=[scalars] * 3,
    )(table, partner, screen, e_occ)


def on_device(integrals, metric, e_occ, e_vir, partner, screen):
    n_occ, n_aux = lax.axis_size("occ"), lax.axis_size("aux")
    groups = n_occ * n_aux
    depth, held, nvir = integrals.shape
    own = held // n_aux
    occ, aux = lax.axis_index("occ"), lax.axis_index("aux")
    device = occ * n_aux + aux

    table = rankings(partner, screen, n_occ, n_aux)

    reader = ((occ + n_occ // 2) % n_occ) * n_aux
    packed = packed_blocks(integrals, reader[None], table, n_aux)

    choices = sorted(set(range(own + 1, 2 * own - 3)) | {2 * own})
    ints, floats, branch = plan(choices, table, partner, screen, e_occ, n_occ, n_aux)

    def chosen(total):
        far, begun, _, _, _, amp, block = moved(packed, metric, e_vir, ints, floats, total, n_occ, n_aux)
        return far, begun, amp, block

    far, begun, amp, block = lax.switch(branch[0], [functools.partial(chosen, total) for total in choices])
    return gradient(far, amp, begun, ints), block


def solution(mesh):
    return jax.shard_map(
        on_device,
        mesh=mesh,
        in_specs=(P("aux", "occ", None), P(), P(), P(), P(BOTH, None), P(BOTH, None)),
        out_specs=(P(None, BOTH, None), P("occ", None)),
        check_vma=False,
    )
```

```python
import functools

import jax
import jax.numpy as jnp
from jax import lax
from jax.experimental import pallas as pl
from jax.experimental.pallas import tpu as pltpu
from jax.sharding import PartitionSpec as P

NOCC = 256
ROUNDS = 2
BOTH = ("occ", "aux")
NT = (((1,), (1,)), ((), ()))
TN = (((0,), (0,)), ((), ()))

MESH = pl.DeviceIdType.MESH


def gamma_kernel(own, at, right, amp, begun, out, rows):
    now = lax.rem(pl.program_id(0), 2)
    for i in range(own):
        term = lax.dot_general(right[at[1, i]], amp[at[3, i]], NT, preferred_element_type=jnp.float32)
        rows[now, i] = (begun[i] + term).astype(rows.dtype)
    out[...] = pltpu.einshape("ipa->pia", rows[1 - now])


def gradient(right, amp, begun, ints):
    slots, naux, nvir = right.shape
    own = amp.shape[0]
    tile = min(256, naux)
    tiles = naux // tile
    this = lambda p, *_: (0, jnp.minimum(p, tiles - 1), 0)
    return pl.pallas_call(
        functools.partial(gamma_kernel, own),
        grid_spec=pltpu.PrefetchScalarGridSpec(
            num_scalar_prefetch=1,
            grid=(tiles + 1,),
            in_specs=[
                pl.BlockSpec((slots, tile, nvir), this),
                pl.BlockSpec(amp.shape, lambda p, *_: (0, 0, 0)),
                pl.BlockSpec((own, tile, nvir), this),
            ],
            out_specs=pl.BlockSpec((tile, own, nvir), lambda p, *_: (jnp.maximum(p - 1, 0), 0, 0)),
            scratch_shapes=[pltpu.VMEM((2, own, tile, nvir), jnp.bfloat16)],
        ),
        out_shape=jax.ShapeDtypeStruct((naux, own, nvir), jnp.bfloat16),
    )(ints, right, amp, begun)


def table_kernel(n_occ, n_aux, partner, screen, table, row, send, recv, local):
    groups = n_occ * n_aux
    own = partner.shape[0]
    me = lax.axis_index("occ") * n_aux + lax.axis_index("aux")

    def wants(k):
        found = jnp.int32(0)
        for i in range(own):
            found = jnp.where((partner[i, 1] == k) & (screen[i, 1] != 0), 1, found)
        return found

    wanted = [wants(k) for k in range(own)]
    total = sum(wanted)
    lend = (total >= own // 2 + 1) & (total < own)
    ahead, slots = jnp.int32(0), []
    for k in range(own):
        behind = jnp.where(lend, total - 1, total) + k - ahead
        last = jnp.where(lend & (ahead == total - 1), own - 1, ahead)
        slots.append(jnp.where(wanted[k] == 1, last, behind))
        ahead = ahead + wanted[k]
    lane = lax.broadcasted_iota(jnp.int32, (1, 128), 1)
    line = jnp.where(lane == 2 * own, total, 0)
    for k in range(own):
        line = line + jnp.where(lane == k, slots[k], 0)
        turned = sum(jnp.where(slots[j] == k, j, 0) for j in range(own))
        line = line + jnp.where(lane == own + k, turned, 0)
    row[...] = line

    barrier = pltpu.get_barrier_semaphore()

    def place(step):
        other = lax.rem(me + step, groups)
        return (other // n_aux, lax.rem(other, n_aux))

    def greet(step, carry):
        pl.semaphore_signal(barrier, inc=1, device_id=place(step), device_id_type=MESH)
        return carry

    lax.fori_loop(1, groups, greet, 0)
    own_row = pltpu.make_async_copy(row, table.at[me], local)
    own_row.start()
    pl.semaphore_wait(barrier, groups - 1)

    def copy(step, came):
        return pltpu.make_async_remote_copy(
            row, table.at[came], send.at[step], recv.at[step], device_id=place(step), device_id_type=MESH
        )

    def start(step, carry):
        copy(step, me).start()
        return carry

    def finish(step, carry):
        copy(step, lax.rem(me - step + groups, groups)).wait()
        return carry

    lax.fori_loop(1, groups, start, 0)
    own_row.wait()
    lax.fori_loop(1, groups, finish, 0)


def rankings(partner, screen, n_occ, n_aux):
    groups = n_occ * n_aux
    scalars = pl.BlockSpec(memory_space=pltpu.SMEM)
    return pl.pallas_call(
        functools.partial(table_kernel, n_occ, n_aux),
        out_shape=jax.ShapeDtypeStruct((groups, 1, 128), jnp.int32),
        in_specs=[scalars] * 2,
        out_specs=pl.BlockSpec(memory_space=pltpu.VMEM),
        scratch_shapes=[
            pltpu.VMEM((1, 128), jnp.int32),
            pltpu.SemaphoreType.DMA((groups,)),
            pltpu.SemaphoreType.DMA((groups,)),
            pltpu.SemaphoreType.DMA(()),
        ],
        compiler_params=pltpu.CompilerParams(collective_id=0, has_side_effects=True),
    )(partner, screen)


def pack_kernel(base, table, x, out, turned):
    n_aux, own = out.shape[:2]
    turned[...] = pltpu.einshape("qja->jqa", x[...])
    for slot in range(n_aux * own):
        reader = base[0] + slot // own
        out[slot // own, slot % own] = turned[slot // own * own + table[reader, 0, own + slot % own]]


def packed_blocks(x, base, table, n_aux):
    depth, held, nvir = x.shape
    own = held // n_aux
    tile = min(32, depth)
    return pl.pallas_call(
        pack_kernel,
        grid_spec=pltpu.PrefetchScalarGridSpec(
            num_scalar_prefetch=2,
            grid=(depth // tile,),
            in_specs=[pl.BlockSpec((tile, held, nvir), lambda q, *_: (q, 0, 0))],
            out_specs=pl.BlockSpec((n_aux, own, tile, nvir), lambda q, *_: (0, 0, q, 0)),
            scratch_shapes=[pltpu.VMEM((held, tile, nvir), x.dtype)],
        ),
        out_shape=jax.ShapeDtypeStruct((n_aux, own, depth, nvir), x.dtype),
    )(base, table, x)


def peer_of(i, step, n_aux):
    return i ^ step if n_aux & (n_aux - 1) == 0 else lax.rem(step + n_aux - i, n_aux)


def shares(total, own):
    caps = ((total + 1) // 2, total // 2)
    spill = tuple(jnp.minimum(own - caps[1 - c], jnp.maximum(caps[c] - 2, 0)) for c in range(2))
    return caps, spill


def fixed_shares(total, own):
    caps = ((total + 1) // 2, total // 2)
    return caps, tuple(min(own - caps[1 - c], max(caps[c] - 2, 0)) for c in range(2))


def move_kernel(
    total, n_occ, n_aux, ints, floats, packed, mixed, col, row,
    far, begun, coeff, wrapped, fills, amp, block_out,
    pool, lent, stage, term, kept_amp, parts, half, sum1, from_side, from_aux, from_z, gathered,
    sent, came, far_sent, far_came, side_sent, side_came, cross_sent, cross_came,
    wrap_sems, local, stored, fold_sent, fold_came, lend_sent, lend_came,
):
    own, depth = packed.shape[1:3]
    naux, nvir = stage.shape
    occ, aux = lax.axis_index("occ"), lax.axis_index("aux")
    core = lax.rem(occ, 2)
    pick = lambda pair: pair[0] + core * (pair[1] - pair[0])
    caps, spills = fixed_shares(total, own)
    cap, cap_mate, spill, spill_mate = pick(caps), pick(caps[::-1]), pick(spills), pick(spills[::-1])
    pooled = total < 2 * own
    aside = own - min(caps) + 1 if pooled else 0
    most_z = n_occ // 2
    mate = (lax.rem(occ + n_occ // 2, n_occ), aux)
    after = (lax.rem(occ + 1, n_occ), aux)
    before = (lax.rem(occ + n_occ - 1, n_occ), aux)
    side = (occ + 1 - 2 * core, aux)
    above = (occ + 2 - 4 * lax.rem(occ // 2, 2), aux)
    peers = [(occ, peer_of(aux, s, n_aux)) for s in range(n_aux)]
    column = [(lax.rem(occ + 2 * k, n_occ), aux) for k in range(most_z)]
    column_before = [(lax.rem(occ + n_occ - 2 * k, n_occ), aux) for k in range(most_z)]

    barrier = pltpu.get_barrier_semaphore()
    greeted = [after, before, side] + peers[1:] + column[1:]
    for device in greeted:
        pl.semaphore_signal(barrier, inc=1, device_id=device, device_id_type=MESH)
    pl.semaphore_wait(barrier, len(greeted))

    def remote(source, target, send, recv, device):
        return pltpu.make_async_remote_copy(source, target, send, recv, device_id=device, device_id_type=MESH)

    wrap = remote(packed.at[n_aux - 1], wrapped, wrap_sems.at[0], wrap_sems.at[1], after)
    wrap.start()

    def part(land, t, q):
        return land.at[t, pl.ds(pl.multiple_of(q * depth, depth), depth)]

    def piece(kind, land, source, t, s, q):
        if s == 0:
            return pltpu.make_async_copy(source, part(land, t, q), local.at[kind, t])
        return remote(source, part(land, t, q), sent.at[kind, t, s], came.at[kind, t, s], peers[s])

    def slot_at(step):
        return jnp.where(step == 1, own - 1, jnp.maximum(step - 1, 0)) if pooled else step

    def send_own(step, carry):
        t = slot_at(step)
        for s in range(n_aux):
            piece(0, pool, packed.at[peers[s][1], t], t, s, aux).start()
        return carry

    def send_near(t, carry):
        for s in range(n_aux):
            to = peers[s][1]

            @pl.when(to == 0)
            def _():
                piece(1, lent, wrapped.at[t], t, s, aux).start()

            @pl.when(to != 0)
            def _():
                piece(1, lent, packed.at[jnp.maximum(to - 1, 0), t], t, s, aux).start()

        return carry

    tile = min(256, naux)

    def put(source, target):
        out = pltpu.make_async_copy(source, target, stored)
        out.start()
        out.wait()

    def transform(kind, land, t):
        for s in range(n_aux):
            move = piece(kind, land, packed.at[0, 0], t, s, peers[s][1])
            move.wait() if s == 0 else move.wait_recv()

        def rows(i, carry):
            at = pl.ds(pl.multiple_of(i * tile, tile), tile)
            stage[at, :] = jnp.dot(mixed[at, :], land[t], preferred_element_type=jnp.float32).astype(stage.dtype)
            return carry

        def back(i, carry):
            at = pl.ds(pl.multiple_of(i * tile, tile), tile)
            land[t, at, :] = stage[at, :]
            return carry

        lax.fori_loop(0, naux // tile, rows, 0)
        lax.fori_loop(0, naux // tile, back, 0)

    def far_copy(source, t):
        return remote(source, far.at[t], far_sent.at[t], far_came.at[t], mate)

    def side_copy(t, x):
        return remote(coeff.at[t], pool.at[own + x], side_sent.at[x], side_came.at[x], side)

    def cross_copy(t, f, place):
        return remote(far.at[t], far.at[place + f], cross_sent.at[f], cross_came.at[f], side)

    def lend_copy():
        return remote(coeff.at[own - 1], pool.at[own + aside], lend_sent.at[0], lend_came.at[0], above)

    def back_copy():
        return remote(far.at[cap - spill], far.at[own], lend_sent.at[1], lend_came.at[1], above)

    def own_slot(step, carry):
        t = slot_at(step)

        @pl.when(step == min(own - 1, 2))
        def _():
            wrap.wait()
            lax.fori_loop(0, own, send_near, 0)

        transform(0, pool, t)
        put(pool.at[t], coeff.at[t])

        @pl.when(t < cap - spill)
        def _():
            far_copy(coeff.at[t], t).start()

        if pooled:

            @pl.when(t >= cap - 1)
            def _():
                side_copy(t, jnp.maximum(t - (cap - 1), 0)).start()

            @pl.when(t == own - 1)
            def _():
                lend_copy().start()

        return carry

    def relay():
        first = cap - spill
        far_copy(coeff.at[first], first).wait_recv()
        back_copy().start()
        cross_copy(first, 0, cap_mate).start()
        far_copy(fills.at[spill - 1], cap - 1).start()

    def near_slot(t, carry):
        transform(1, lent, t)
        if pooled:

            @pl.when(t == (own - 3 if total <= own + 2 else own - 2))
            def _():
                relay()

        return carry

    lax.fori_loop(0, own, send_own, 0)
    lax.fori_loop(0, own, own_slot, 0)

    def side_wait(x, carry):
        side_copy(0, x).wait_recv()
        return carry

    if pooled:
        lax.fori_loop(0, own - cap_mate + 1, side_wait, 0)
        lend_copy().wait_recv()

    def fill(f, carry):
        def copy(i, inner):
            at = pl.ds(pl.multiple_of(i * tile, tile), tile)
            stage[at, :] = pool[ints[2, f], at, :]
            return inner

        lax.fori_loop(0, naux // tile, copy, 0)
        put(stage, fills.at[f])
        @pl.when(f < spill - 1)
        def _():
            far_copy(fills.at[f], cap - spill + f).start()

        return carry

    lax.fori_loop(0, spill, fill, 0)
    lax.fori_loop(0, own, near_slot, 0)

    parts[...] = jnp.zeros_like(parts)

    def amplitude(left, right, kept, gap):
        both = lax.dot_general(left, right, TN, preferred_element_type=jnp.float32)
        block = (kept * both / (col[...] + row[...] - gap[0] - gap[1])).astype(amp.dtype)
        square = lax.dot_general(block, block, NT, preferred_element_type=jnp.float32)
        parts[...] += square.reshape(parts.shape)
        return block

    def pair0(i, carry):
        kept_amp[...] = amplitude(pool[ints[4, i]], lent[ints[0, i]], floats[0, i], (floats[2, i], floats[4, i]))

        def rows(k, inner):
            at = pl.ds(pl.multiple_of(k * tile, tile), tile)
            term[...] = lax.dot_general(
                lent[ints[0, i], at, :], kept_amp[...], NT, preferred_element_type=jnp.float32
            )
            put(term, begun.at[i, at])
            return inner

        lax.fori_loop(0, naux // tile, rows, 0)
        return carry

    lax.fori_loop(0, own, pair0, 0)

    def pair1(m, carry):
        kept_amp[...] = amplitude(pool[ints[5, m]], lent[ints[6, m]], floats[1, m], (floats[3, m], floats[5, m]))
        put(kept_amp, amp.at[m])
        return carry

    def arrive(u, carry):
        @pl.when(u != cap - spill if pooled else u >= 0)
        def _():
            far_copy(coeff.at[u], u).wait_recv()

        if pooled:

            @pl.when(u > cap - spill)
            def _():
                cross_copy(u, jnp.maximum(u - (cap - spill), 0), cap_mate).start()

        put(far.at[u], lent.at[u])
        if pooled:

            @pl.when(u >= 1)
            def _():
                pair1(jnp.maximum(u - 1, 0), 0)

        return carry

    def crossed(f, carry):
        cross_copy(0, f, cap).wait_recv()
        put(far.at[cap + f], lent.at[cap + f])
        return carry

    lax.fori_loop(0, cap, arrive, 0)
    if pooled:
        back_copy().wait_recv()
        put(far.at[own], lent.at[own])
        lax.fori_loop(0, spill_mate, crossed, 0)
    lax.fori_loop(cap - 1 if pooled else 0, own, pair1, 0)

    fold = lambda k, source, target, device: remote(source, target, fold_sent.at[k], fold_came.at[k], device)
    swap = fold(0, parts.at[:, 1 - core], from_side, side)
    swap.start()
    swap.wait()
    half[...] = parts[:, core] + from_side[...]
    moves = [fold(s, half.at[:, peers[s][1]], from_aux.at[s - 1], peers[s]) for s in range(1, n_aux)]
    for move in moves:
        move.start()
    for move in moves:
        move.wait()
    sum1[...] = half[:, aux] + jnp.sum(from_aux[...], axis=0)
    moves = []
    for k in range(1, most_z):
        moves.append(fold(n_aux + k - 1, sum1.at[column[k][0] // 2], from_z.at[k - 1], column[k]))
    for move in moves:
        move.start()
    for move in moves:
        move.wait()
    gathered[aux] = (sum1[occ // 2] + jnp.sum(from_z[...], axis=0)) / NOCC
    base = n_aux + most_z - 2
    moves = [fold(base + s, gathered.at[aux], gathered.at[aux], peers[s]) for s in range(1, n_aux)]
    for move in moves:
        move.start()
    for s, move in enumerate(moves):
        move.wait_send()
        fold(base + s + 1, gathered.at[aux], gathered.at[peers[s + 1][1]], peers[s + 1]).wait_recv()
    block_out[...] = gathered[...].reshape(block_out.shape)

    def drain(t, carry):
        for kind, land in ((0, pool), (1, lent)):
            for s in range(1, n_aux):
                piece(kind, land, packed.at[0, 0], t, s, aux).wait_send()
        return carry

    def side_drain(x, carry):
        side_copy(0, x).wait_send()
        return carry

    def far_drain(t, carry):
        far_copy(coeff.at[t], t).wait_send()
        return carry

    def cross_drain(f, carry):
        cross_copy(0, f, cap_mate).wait_send()
        return carry

    lax.fori_loop(0, own, drain, 0)
    lax.fori_loop(0, cap, far_drain, 0)
    if pooled:
        lax.fori_loop(0, own - cap + 1, side_drain, 0)
        lax.fori_loop(0, spill, cross_drain, 0)
        lend_copy().wait_send()
        back_copy().wait_send()


def moved(packed, mixed, e_vir, ints, floats, total, n_occ, n_aux):
    _, own, depth, nvir = packed.shape
    naux = depth * n_aux
    caps, spills = fixed_shares(total, own)
    spill, aside = max(1, *spills), own - min(caps) + 1 if total < 2 * own else 0
    anywhere = pl.BlockSpec(memory_space=pl.ANY)
    fast = pl.BlockSpec(memory_space=pltpu.VMEM)
    scalars = pl.BlockSpec(memory_space=pltpu.SMEM)
    kind = packed.dtype
    dma = pltpu.SemaphoreType.DMA
    wide = lambda count: jax.ShapeDtypeStruct((count, naux, nvir), kind)
    most_z, thin = n_occ // 2, nvir // (n_occ * n_aux)
    single = lambda *lead: pltpu.VMEM(lead + (thin, nvir), jnp.float32)
    folds = 2 * n_aux + most_z - 1
    return pl.pallas_call(
        functools.partial(move_kernel, total, n_occ, n_aux),
        out_shape=[
            wide(own + 1),
            jax.ShapeDtypeStruct((own, naux, nvir), jnp.float32),
            wide(own),
            jax.ShapeDtypeStruct((own, depth, nvir), kind),
            wide(spill),
            jax.ShapeDtypeStruct((own, nvir, nvir), kind),
            jax.ShapeDtypeStruct((nvir // n_occ, nvir), jnp.float32),
        ],
        in_specs=[scalars] * 2 + [anywhere, fast, fast, fast],
        out_specs=[anywhere] * 6 + [fast],
        scratch_shapes=[
            pltpu.VMEM((own + aside + 1, naux, nvir), kind),
            pltpu.VMEM((own + 1, naux, nvir), kind),
            pltpu.VMEM((naux, nvir), kind),
            pltpu.VMEM((min(256, naux), nvir), jnp.float32),
            pltpu.VMEM((nvir, nvir), kind),
            single(most_z, 2, n_aux),
            single(most_z, n_aux),
            single(most_z),
            single(most_z, n_aux),
            single(n_aux - 1, most_z),
            single(most_z - 1),
            single(n_aux),
            dma((2, own, n_aux)),
            dma((2, own, n_aux)),
            dma((own,)),
            dma((own,)),
            dma((max(1, aside),)),
            dma((max(1, aside),)),
            dma((spill,)),
            dma((spill,)),
            dma((2,)),
            dma((2, own)),
            dma(()),
            dma((folds,)),
            dma((folds,)),
            dma((2,)),
            dma((2,)),
        ],
        compiler_params=pltpu.CompilerParams(
            collective_id=total, has_side_effects=True, vmem_limit_bytes=67043328
        ),
    )(ints, floats, packed, mixed, e_vir[:, None], e_vir[None, :])


def lending(total, own, wanted):
    caps, spill = shares(total, own)
    over = [wanted[z][0] + wanted[z][1] - total for z in range(2)]
    flag = lambda test: jnp.where(test, 1, 0)
    lends = []
    for z in range(2):
        big = [wanted[z][c] > caps[c] for c in range(2)]
        one, two = over[z] == 1, over[z] == 2
        lends.append([flag((one & big[0]) | two), flag((one & jnp.logical_not(big[0])) | two)])
    fine, items, excess = True, [], []
    for z in range(2):
        fine = fine & (over[z] <= 2)
        for c in range(2):
            fine = fine & ((lends[z][c] == 0) | (wanted[z][c] > caps[c]))
        items.append(
            [lends[1 - z][c] + jnp.maximum(wanted[z][c] - caps[c] + spill[c], 0) - lends[z][c] for c in range(2)]
        )
        excess.append([jnp.maximum(items[z][c] - spill[c], 0) for c in range(2)])
        for c in range(2):
            fine = fine & (jnp.minimum(items[z][c], spill[c]) + excess[z][1 - c] <= spill[c])
            fine = fine & ((lends[z][0] + lends[z][1] == 0) | (lends[1 - z][c] == 0))
    return lends, items, excess, fine


def plan_kernel(choices, n_occ, n_aux, table, partner, screen, e_occ, ints, floats, branch):
    groups = n_occ * n_aux
    own = partner.shape[0]
    occ, aux = lax.axis_index("occ"), lax.axis_index("aux")
    device = occ * n_aux + aux
    far_by = groups // 2
    reader = lambda source: lax.rem(source + far_by, groups)
    slot_of = lambda source, orbital: table[reader(source), 0, orbital]

    def counts(first):
        count = lambda o: table[reader(o * n_aux + aux_of), 0, 2 * own]
        aux_of = lax.rem(first, n_aux)
        row = first // n_aux
        return [[count(row + 2 * z + c) for c in range(2)] for z in range(2)]

    chosen, total = jnp.int32(0), jnp.int32(choices[0])
    for k in range(1, len(choices)):

        def quad(q, good):
            first = q // n_aux * 4 * n_aux + lax.rem(q, n_aux)
            return good & jnp.where(lending(choices[k - 1], own, counts(first))[3], 1, 0)

        over = lax.fori_loop(0, groups // 4, quad, jnp.int32(1)) == 0
        still = over & (chosen == k - 1)
        chosen = jnp.where(still, k, chosen)
        total = jnp.where(still, choices[k], total)
    branch[0] = chosen
    pooled = total < 2 * own
    caps, spills = shares(total, own)
    core = lax.rem(occ, 2)
    level = lax.rem(occ // 2, 2)
    by_core = lambda pair, c: jnp.where(c == 0, pair[0], pair[1])
    at = lambda grid, z, c: by_core([by_core(grid[0], c), by_core(grid[1], c)], z)
    cap, cap_mate = by_core(caps, core), by_core(caps, 1 - core)
    spill, spill_mate = by_core(spills, core), by_core(spills, 1 - core)
    aside = own - caps[1] + 1
    many = own // 2 + 1

    def shared_slot(item, first_shared, wanted):
        lent = (wanted >= many) & (item == wanted - 1 - first_shared)
        return jnp.where(lent, own - 1, first_shared + item)

    wanted = counts((occ - 2 * level - core) * n_aux + aux)
    lends, items, excess, _ = lending(total, own, wanted)
    carries, mine, theirs = at(lends, 1 - level, core), at(items, level, core), at(excess, level, 1 - core)
    wanted_own, wanted_side = at(wanted, level, core), at(wanted, level, 1 - core)
    side_carries = at(lends, 1 - level, 1 - core)
    for f in range(own):
        own_item = shared_slot(f - carries, cap - spill, wanted_own)
        k = f - mine
        side_slot = shared_slot(spill_mate - side_carries + k, cap_mate - spill_mate, wanted_side)
        side_item = jnp.where(k < theirs, own + side_slot - (cap_mate - 1), 0)
        item = jnp.where(f < mine, own_item, side_item)
        item = jnp.where((f == 0) & (carries == 1), own + aside, item)
        ints[2, f] = jnp.where(pooled, jnp.clip(item, 0, own + aside), 0)

    near, far = lax.rem(device + groups - 1, groups), lax.rem(device + groups - far_by, groups)
    source_occ = far // n_aux
    wanted = counts((source_occ - 2 * level - core) * n_aux + aux)
    lends, items, _, _ = lending(total, own, wanted)
    lent_one, carries = at(lends, level, core), at(lends, 1 - level, core)
    wanted_own = at(wanted, level, core)
    side_items = jnp.minimum(at(items, level, 1 - core), spill_mate)

    def far_slot(slot):
        special = (slot == own - 1) & (wanted_own >= many)
        item = jnp.where(special, wanted_own - 1 - (cap - spill), slot - (cap - spill))
        f = carries + item
        shared = jnp.where(f < spill, cap - spill + f, cap + side_items + f - spill)
        place = jnp.where(special & (lent_one == 1), own, shared)
        place = jnp.where(slot < cap - spill, slot, place)
        return jnp.clip(place, 0, own)

    found = [far_slot(slot_of(far, partner[i, 1])) for i in range(own)]
    found = [jnp.where(screen[i, 1] != 0, found[i], 0) for i in range(own)]
    keys = [jnp.where(screen[i, 1] != 0, found[i], own + 1) for i in range(own)]
    for i in range(own):
        ints[0, i] = slot_of(near, partner[i, 0])
        ints[1, i] = found[i]
        where = jnp.int32(0)
        for other in range(own):
            if other != i:
                ahead = keys[other] < keys[i] if other > i else keys[other] <= keys[i]
                where = where + jnp.where(ahead, 1, 0)
        ints[3, i] = where
        mine = slot_of(device, i)
        ints[4, i] = mine
        ints[5, where] = mine
        ints[6, where] = found[i]
        floats[0, i] = screen[i, 0].astype(jnp.float32)
        floats[1, where] = screen[i, 1].astype(jnp.float32)
        energy = e_occ[device * own + i]
        floats[2, i] = energy
        floats[3, where] = energy
        floats[4, i] = e_occ[near * own + partner[i, 0]]
        floats[5, where] = e_occ[far * own + partner[i, 1]]


def plan(choices, table, partner, screen, e_occ, n_occ, n_aux):
    own = partner.shape[0]
    scalars = pl.BlockSpec(memory_space=pltpu.SMEM)
    return pl.pallas_call(
        functools.partial(plan_kernel, choices, n_occ, n_aux),
        out_shape=[
            jax.ShapeDtypeStruct((7, own), jnp.int32),
            jax.ShapeDtypeStruct((6, own), jnp.float32),
            jax.ShapeDtypeStruct((1,), jnp.int32),
        ],
        in_specs=[scalars] * 4,
        out_specs=[scalars] * 3,
    )(table, partner, screen, e_occ)


def on_device(integrals, metric, e_occ, e_vir, partner, screen):
    n_occ, n_aux = lax.axis_size("occ"), lax.axis_size("aux")
    groups = n_occ * n_aux
    depth, held, nvir = integrals.shape
    own = held // n_aux
    occ, aux = lax.axis_index("occ"), lax.axis_index("aux")
    device = occ * n_aux + aux

    table = rankings(partner, screen, n_occ, n_aux)

    reader = ((occ + n_occ // 2) % n_occ) * n_aux
    packed = packed_blocks(integrals, reader[None], table, n_aux)

    choices = sorted(set(range(own + 1, 2 * own - 3)) | {2 * own})
    ints, floats, branch = plan(choices, table, partner, screen, e_occ, n_occ, n_aux)

    def chosen(total):
        far, begun, _, _, _, amp, block = moved(packed, metric, e_vir, ints, floats, total, n_occ, n_aux)
        return far, begun, amp, block

    far, begun, amp, block = lax.switch(branch[0], [functools.partial(chosen, total) for total in choices])
    return gradient(far, amp, begun, ints), block


def solution(mesh):
    return jax.shard_map(
        on_device,
        mesh=mesh,
        in_specs=(P("aux", "occ", None), P(), P(), P(), P(BOTH, None), P(BOTH, None)),
        out_specs=(P(None, BOTH, None), P("occ", None)),
        check_vma=False,
    )
```
